32 devices in a mesh: dp: 1 (over z), ffn: 4 (over y), emb: 8 (over x, core).
Axes of the slice: x: 4, y: 4, z: 1, core: 2. Of those that a mesh axis runs over, the one named last changes fastest.
The devices are a block of a 4x4x8 slice.
Arguments:
- hidden: bfloat16 [2048, 2048], P('dp', 'emb')
- norm_pre: bfloat16 [2048], P('emb')
- norm_post: bfloat16 [2048], P('emb')
- w_router: bfloat16 [2048, 64], P('emb')
- w_gate: bfloat16 [64, 2048, 1024], P(None, 'emb', 'ffn')
- w_up: bfloat16 [64, 2048, 1024], P(None, 'emb', 'ffn')
- w_down: bfloat16 [64, 1024, 2048], P(None, 'ffn', 'emb')
- choice: int32 [2048, 8], P('dp')
Outputs:
- output: bfloat16 [2048, 2048], P('dp', 'emb')
All inputs are finite; a program needn't handle non-finite values.
Results may differ from the reference program's by a relative error of at most 0.0143155.
Values are sent between devices in bfloat16 or wider.
A program may use at most 768 MiB of HBM per device.

```python
import math
import jax
import jax.numpy as jnp
from jax import lax

D = 2048
E = 64
F = 1024
TOP = 8
B = 2048
CAP = 2 * B * TOP // E
EPS = 1e-5


def width_profile(key, size):
    slope = jax.random.uniform(key, (), minval=1.5, maxval=2.5)
    return jnp.exp(slope * (jnp.arange(size, dtype=jnp.float32) / size - 0.5))


def draw_choice(key):
    key_hot, key_perm, key_score = jax.random.split(key, 3)
    hot_id = jax.random.randint(key_hot, (), 0, E)
    forced = jax.random.permutation(key_perm, B) < (3 * B) // 4
    expert_ids = jnp.arange(E)
    score = jax.random.randint(key_score, (B, E), 1, 1048576) * E + expert_ids[None, :]
    score = jnp.where(forced[:, None] & (expert_ids[None, :] == hot_id), 0, score)
    return jnp.argsort(score, axis=1, stable=True)[:, :TOP].astype(jnp.int32)


def setup_inputs(seed: int = 0, part: int = 0) -> dict:
    base_key = jax.random.key(seed)
    part_keys = jax.random.split(jax.random.fold_in(base_key, part), 4)
    shared_keys = jax.random.split(base_key, 7)
    row_scale = jnp.exp(0.5 * jax.random.normal(part_keys[0], (B, 1)))
    hidden = jax.random.normal(part_keys[1], (B, D)) * row_scale * width_profile(part_keys[2], D)[None, :]
    norm_pre = 1.0 + 0.3 * jax.random.normal(shared_keys[0], (D,))
    norm_post = 1.0 + 0.3 * jax.random.normal(shared_keys[1], (D,))
    w_router = jax.random.normal(shared_keys[2], (D, E)) * (1.5 / math.sqrt(D))
    w_gate = jax.random.normal(shared_keys[3], (E, D, F)) * (1.0 / math.sqrt(D))
    w_up = jax.random.normal(shared_keys[4], (E, D, F)) * (1.0 / math.sqrt(D))
    w_down = jax.random.normal(shared_keys[5], (E, F, D)) * (1.0 / math.sqrt(F)) * width_profile(shared_keys[6], D)[None, None, :]
    return {
        'hidden': hidden.astype(jnp.bfloat16),
        'norm_pre': norm_pre.astype(jnp.bfloat16),
        'norm_post': norm_post.astype(jnp.bfloat16),
        'w_router': w_router.astype(jnp.bfloat16),
        'w_gate': w_gate.astype(jnp.bfloat16),
        'w_up': w_up.astype(jnp.bfloat16),
        'w_down': w_down.astype(jnp.bfloat16),
        'choice': draw_choice(part_keys[3]),
    }


def route_tokens(choice, router_prob):
    onehot = (choice[:, :, None] == jnp.arange(E)[None, None, :]).astype(jnp.int32)
    assigned = jnp.sum(onehot, axis=1)
    before = jnp.cumsum(assigned, axis=0) - assigned
    slot_idx = jnp.sum(onehot * before[:, None, :], axis=2)
    position = jnp.where(slot_idx < CAP, choice * CAP + slot_idx, E * CAP)
    gate_val = jnp.take_along_axis(router_prob, choice, axis=1)
    flat_pos = position.reshape(-1)
    token_ids = jnp.repeat(jnp.arange(B, dtype=jnp.int32), TOP)
    slot_token = jnp.full((E * CAP,), B, jnp.int32).at[flat_pos].set(token_ids, mode='drop')
    slot_gate = jnp.zeros((E * CAP,), jnp.float32).at[flat_pos].set(gate_val.reshape(-1), mode='drop')
    return position, slot_token, slot_gate


def expert_ffn(operands):
    slot_rows, gate_w, up_w, down_w = operands
    z_gate = jnp.dot(slot_rows, gate_w, preferred_element_type=jnp.float32).astype(jnp.bfloat16)
    z_up = jnp.dot(slot_rows, up_w, preferred_element_type=jnp.float32).astype(jnp.bfloat16)
    act_val = (jax.nn.gelu(z_gate.astype(jnp.float32), approximate=True) * z_up.astype(jnp.float32)).astype(jnp.bfloat16)
    return jnp.dot(act_val, down_w, preferred_element_type=jnp.float32).astype(jnp.bfloat16)


def reference(hidden, norm_pre, norm_post, w_router, w_gate, w_up, w_down, choice):
    hid_f32 = hidden.astype(jnp.float32)
    inv_pre = lax.rsqrt(jnp.mean(hid_f32 * hid_f32, axis=1, keepdims=True) + EPS)
    normed = (hid_f32 * inv_pre * norm_pre.astype(jnp.float32)).astype(jnp.bfloat16)
    logits = jnp.dot(normed, w_router, preferred_element_type=jnp.float32)
    router_prob = jax.nn.softmax(logits, axis=1)
    position, slot_token, slot_gate = route_tokens(choice, router_prob)
    expert_in = jnp.take(normed, slot_token, axis=0, mode='fill', fill_value=0).reshape(E, CAP, D)
    expert_out = lax.map(expert_ffn, (expert_in, w_gate, w_up, w_down))
    weighted = (expert_out.reshape(E * CAP, D).astype(jnp.float32) * slot_gate[:, None]).astype(jnp.bfloat16)
    picked = jnp.take(weighted, position, axis=0, mode='fill', fill_value=0)
    mix_sum = jnp.sum(picked.astype(jnp.float32), axis=1)
    inv_post = lax.rsqrt(jnp.mean(mix_sum * mix_sum, axis=1, keepdims=True) + EPS)
    return (hid_f32 + mix_sum * inv_post * norm_post.astype(jnp.float32)).astype(jnp.bfloat16)
```

```python
import functools

import jax
import jax.numpy as jnp
from jax import lax
from jax.experimental import pallas as pl
from jax.experimental.pallas import tpu as pltpu
from jax.sharding import PartitionSpec as P

EPS = 1e-5
LANE = 128
F_CHUNKS = 2
ROW_BLOCK = 272
EXPERT_BATCH = 4
VMEM_BYTES = 60 * 1024 * 1024
F32 = jnp.float32
BF16 = jnp.bfloat16


def cost(flops, nbytes):
    return pl.CostEstimate(flops=int(flops), bytes_accessed=int(nbytes), transcendentals=0)


def onehot_pieces(pos_row, rows_hi):
    tokens = pos_row.shape[1]
    hi = jnp.floor(pos_row * (1.0 / LANE))
    lo = pos_row - hi * LANE
    hi_iota = lax.broadcasted_iota(jnp.int32, (rows_hi, tokens), 0).astype(F32)
    lo_iota = lax.broadcasted_iota(jnp.int32, (LANE, tokens), 0).astype(F32)
    return hi == hi_iota, lo == lo_iota


def route_kernel(capacity, experts, choice_ref, tok_ref, seg_ref, pos_ref):
    top_k, tokens = choice_ref.shape
    rows_hi = tok_ref.shape[0]
    rows = rows_hi * LANE
    blk = 256
    e_iota = lax.broadcasted_iota(jnp.int32, (experts, tokens), 0)
    assigned = jnp.zeros((experts, tokens), F32)
    for k in range(top_k):
        assigned += jnp.where(choice_ref[k:k + 1, :] == e_iota, 1.0, 0.0)
    r_i = lax.broadcasted_iota(jnp.int32, (blk, blk), 0)
    c_i = lax.broadcasted_iota(jnp.int32, (blk, blk), 1)
    tri = jnp.where(r_i < c_i, 1.0, 0.0).astype(BF16)
    carry = jnp.zeros((experts, 1), F32)
    before = []
    for b in range(tokens // blk):
        part = assigned[:, b * blk:(b + 1) * blk]
        within = jnp.dot(part.astype(BF16), tri, preferred_element_type=F32)
        before.append(within + carry)
        carry = carry + jnp.sum(part, axis=1, keepdims=True)
    before = jnp.concatenate(before, axis=1)
    kept = jnp.broadcast_to(jnp.minimum(carry, float(capacity)), (experts, LANE))
    kept_hi = jnp.floor(kept * (1.0 / 16.0))
    kept_lo = kept - kept_hi * 16.0
    er = lax.broadcasted_iota(jnp.int32, (experts, experts), 0)
    ec = lax.broadcasted_iota(jnp.int32, (experts, experts), 1)
    low = jnp.where(ec < er, 1.0, 0.0).astype(BF16)
    start = 16.0 * jnp.dot(low, kept_hi.astype(BF16), preferred_element_type=F32)
    start = start + jnp.dot(low, kept_lo.astype(BF16), preferred_element_type=F32)
    end = start + kept
    fill = jnp.zeros((LANE - experts, LANE), F32)
    start_t = jnp.transpose(jnp.concatenate([start, fill], axis=0))
    end_t = jnp.transpose(jnp.concatenate([end, fill], axis=0))
    seg_ref[0:1, :] = start_t[0:1, :].astype(jnp.int32)
    lane = lax.broadcasted_iota(jnp.int32, (1, LANE), 1)
    seg_ref[1:2, :] = jnp.where(lane == experts - 1, rows, end_t[0:1, :].astype(jnp.int32))
    value = jnp.where(before < capacity, before + start[:, 0:1], float(rows))
    t_val = lax.broadcasted_iota(jnp.int32, (1, tokens), 1) + 1
    t_hi = (t_val // 16).astype(F32)
    t_lo = (t_val % 16).astype(F32)
    acc = jnp.zeros((rows_hi, 2 * LANE), F32)
    for k in range(top_k):
        hit = choice_ref[k:k + 1, :] == e_iota
        pos = jnp.sum(jnp.where(hit, value, 0.0), axis=0, keepdims=True)
        pos_ref[k:k + 1, :] = pos
        is_hi, is_lo = onehot_pieces(pos, rows_hi)
        left = jnp.where(is_hi, 1.0, 0.0).astype(BF16)
        right = jnp.concatenate([jnp.where(is_lo, t_hi, 0.0), jnp.where(is_lo, t_lo, 0.0)], axis=0).astype(BF16)
        acc += lax.dot_general(left, right, (((1,), (1,)), ((), ())), preferred_element_type=F32)
    tok_ref[...] = (16.0 * acc[:, :LANE] + acc[:, LANE:]).astype(jnp.int32) - 1


def route(choice, experts, capacity):
    tokens, top_k = choice.shape
    rows_hi = tokens * top_k // LANE
    return pl.pallas_call(
        functools.partial(route_kernel, capacity, experts),
        out_shape=(
            jax.ShapeDtypeStruct((rows_hi, LANE), jnp.int32),
            jax.ShapeDtypeStruct((2, LANE), jnp.int32),
            jax.ShapeDtypeStruct((top_k, tokens), F32),
        ),
        compiler_params=pltpu.CompilerParams(vmem_limit_bytes=VMEM_BYTES),
        cost_estimate=cost(10e9, 1e5),
        name='route',
    )(choice.T)


def norm_kernel(hid_ref, inv_ref, pre_ref, wr_ref, b_ref, logit_ref):
    width = hid_ref.shape[1]
    for i in range(inv_ref.shape[0]):
        col = jnp.concatenate([column_of(inv_ref[i:i + 1, :])] * (width // LANE), axis=1)
        part = slice(i * LANE, (i + 1) * LANE)
        b_ref[part, :] = (hid_ref[part, :].astype(F32) * col * pre_ref[...].astype(F32)).astype(BF16)
    b = b_ref[...]
    logit_ref[...] = lax.dot_general(wr_ref[...], b, (((0,), (1,)), ((), ())), preferred_element_type=F32)


def norm_logits(hidden, inv_pre, norm_pre, w_router):
    tokens, width = hidden.shape
    experts = w_router.shape[1]
    return pl.pallas_call(
        norm_kernel,
        out_shape=(
            jax.ShapeDtypeStruct((tokens, width), BF16),
            jax.ShapeDtypeStruct((experts, tokens), F32),
        ),
        compiler_params=pltpu.CompilerParams(vmem_limit_bytes=VMEM_BYTES),
        cost_estimate=cost(5e9, 3e6),
        name='norm_logits',
    )(hidden, inv_pre.reshape(tokens // LANE, LANE), norm_pre.reshape(1, width), w_router)


def column_of(row):
    return jnp.transpose(jnp.broadcast_to(row, (LANE, LANE)))


def dispatch_kernel(tok_ref, b_ref, x_ref):
    i = pl.program_id(0)
    tokens = b_ref.shape[0]
    rows = x_ref.shape[0]
    lane = lax.broadcasted_iota(jnp.int32, (LANE, LANE), 1)
    strips = []
    for q in range(rows // LANE):
        col = column_of(tok_ref[pl.ds(i * (rows // LANE) + q, 1), :])
        strips.append(jnp.concatenate(
            [jnp.where(col == lane + j * LANE, 1.0, 0.0).astype(BF16) for j in range(tokens // LANE)], axis=1))
    pick = jnp.concatenate(strips, axis=0)
    x_ref[...] = jnp.dot(pick, b_ref[...], preferred_element_type=F32).astype(BF16)


def dispatch(tok, b):
    tokens, width = b.shape
    rows = tok.size
    blk = 512
    return pl.pallas_call(
        dispatch_kernel,
        out_shape=jax.ShapeDtypeStruct((rows, width), BF16),
        grid=(rows // blk,),
        in_specs=[
            pl.BlockSpec(tok.shape, lambda i: (0, 0)),
            pl.BlockSpec((tokens, width), lambda i: (0, 0)),
        ],
        out_specs=pl.BlockSpec((blk, width), lambda i: (i, 0)),
        compiler_params=pltpu.CompilerParams(vmem_limit_bytes=VMEM_BYTES),
        cost_estimate=cost(2 * rows * tokens * width, rows * width * 2),
        name='dispatch',
    )(tok, b)


def grouped(seg_ref, step, in_refs, weights, out_ref):
    total = out_ref.shape[0]
    batch = len(weights)

    def block(e, w, offset):
        s = seg_ref[0, e]
        r0 = pl.multiple_of(jnp.minimum((s // 16) * 16 + offset, total - ROW_BLOCK), 16)
        parts = [r[pl.ds(r0, ROW_BLOCK), :] for r in in_refs]
        src = parts[0] if len(parts) == 1 else jnp.concatenate(parts, axis=1)
        new = jnp.dot(src, w(), preferred_element_type=F32).astype(BF16)
        return s, r0, new

    def put(s, r0, new):
        row = r0 + lax.broadcasted_iota(jnp.int32, new.shape, 0)
        out_ref[pl.ds(r0, ROW_BLOCK), :] = jnp.where(row >= s, new, out_ref[pl.ds(r0, ROW_BLOCK), :])

    long = jnp.bool_(False)
    for q in range(batch):
        e = step * batch + q
        long = jnp.logical_or(long, seg_ref[1, e] - (seg_ref[0, e] // 16) * 16 > ROW_BLOCK)

    @pl.when(jnp.logical_not(long))
    def short_segments():
        for item in [block(step * batch + q, weights[q], 0) for q in range(batch)]:
            put(*item)

    @pl.when(long)
    def long_segments():
        for q in range(batch):
            e = step * batch + q
            count = (seg_ref[1, e] - (seg_ref[0, e] // 16) * 16 + ROW_BLOCK - 1) // ROW_BLOCK

            def body(j, carry):
                put(*block(e, weights[q], j * ROW_BLOCK))
                return carry

            lax.fori_loop(0, count, body, 0)


def up_kernel(seg_ref, x_ref, wg_ref, wu_ref, z_ref):
    pick = lambda q: lambda: jnp.concatenate([wg_ref[q], wu_ref[q]], axis=1)
    grouped(seg_ref, pl.program_id(0), [x_ref], [pick(q) for q in range(wg_ref.shape[0])], z_ref)


def expert_up(seg, x, w_gate, w_up, chunk, chunks):
    rows, width = x.shape
    experts, _, ffn = w_gate.shape
    part = ffn // chunks
    w_spec = pl.BlockSpec((EXPERT_BATCH, width, part), lambda e, seg: (e, 0, chunk))
    return pl.pallas_call(
        up_kernel,
        out_shape=jax.ShapeDtypeStruct((rows, 2 * part), BF16),
        grid_spec=pltpu.PrefetchScalarGridSpec(
            num_scalar_prefetch=1,
            grid=(experts // EXPERT_BATCH,),
            in_specs=[pl.BlockSpec((rows, width), lambda e, seg: (0, 0), pipeline_mode=pl.Buffered(1)), w_spec, w_spec],
            out_specs=pl.BlockSpec((rows, 2 * part), lambda e, seg: (0, 0), pipeline_mode=pl.Buffered(1)),
        ),
        compiler_params=pltpu.CompilerParams(vmem_limit_bytes=VMEM_BYTES),
        cost_estimate=cost(8 * rows * width * part, 4 * rows * width),
        name='expert_up',
    )(seg, x, w_gate, w_up)


def gate_kernel(logit_ref, choice_ref, pos_ref, gate_ref):
    experts, tokens = logit_ref.shape
    top_k = choice_ref.shape[0]
    rows_hi = gate_ref.shape[0]
    logits = logit_ref[...]
    grown = jnp.exp(logits - jnp.max(logits, axis=0, keepdims=True))
    prob = grown / jnp.sum(grown, axis=0, keepdims=True)
    e_iota = lax.broadcasted_iota(jnp.int32, (experts, tokens), 0)
    acc = jnp.zeros((rows_hi, 3 * LANE), F32)
    for k in range(top_k):
        hit = choice_ref[k:k + 1, :] == e_iota
        gate = jnp.sum(jnp.where(hit, prob, 0.0), axis=0, keepdims=True)
        is_hi, is_lo = onehot_pieces(pos_ref[k:k + 1, :], rows_hi)
        left = jnp.where(is_hi, 1.0, 0.0).astype(BF16)
        pieces = []
        rest = gate
        for _ in range(3):
            piece = rest.astype(BF16).astype(F32)
            rest = rest - piece
            pieces.append(jnp.where(is_lo, piece, 0.0).astype(BF16))
        right = jnp.concatenate(pieces, axis=0)
        acc += lax.dot_general(left, right, (((1,), (1,)), ((), ())), preferred_element_type=F32)
    gate_ref[...] = acc[:, :LANE] + acc[:, LANE:2 * LANE] + acc[:, 2 * LANE:]


def gates_of_rows(logits, choice_t, pos):
    top_k, tokens = choice_t.shape
    rows_hi = tokens * top_k // LANE
    return pl.pallas_call(
        gate_kernel,
        out_shape=jax.ShapeDtypeStruct((rows_hi, LANE), F32),
        compiler_params=pltpu.CompilerParams(vmem_limit_bytes=VMEM_BYTES),
        cost_estimate=cost(10e9, 1e5),
        name='gates',
    )(logits, choice_t, pos)


def down_kernel(chunks, seg_ref, tok_ref, gate_ref, *refs):
    g_refs = refs[:chunks]
    w_ref, m_ref, y_ref = refs[chunks:]
    tokens, width = m_ref.shape
    rows = y_ref.shape[0]
    pick = lambda q: lambda: w_ref[q]
    grouped(seg_ref, pl.program_id(0), g_refs, [pick(q) for q in range(w_ref.shape[0])], y_ref)

    @pl.when(pl.program_id(0) == pl.num_programs(0) - 1)
    def combine():
        blk = 512
        t_iota = lax.broadcasted_iota(jnp.int32, (tokens, LANE), 0)
        m_ref[...] = jnp.zeros_like(m_ref)

        def body(i, carry):
            scaled, picks = [], []
            for q in range(blk // LANE):
                hi = i * (blk // LANE) + q
                col = column_of(gate_ref[pl.ds(hi, 1), :])
                col = jnp.concatenate([col] * (width // LANE), axis=1)
                r0 = pl.multiple_of(hi * LANE, LANE)
                scaled.append((y_ref[pl.ds(r0, LANE), :].astype(F32) * col).astype(BF16))
                picks.append(jnp.where(t_iota == tok_ref[pl.ds(hi, 1), :], 1.0, 0.0).astype(BF16))
            u = jnp.concatenate(scaled, axis=0)
            pick = jnp.concatenate(picks, axis=1)
            m_ref[...] += jnp.dot(pick, u, preferred_element_type=F32)
            return carry

        lax.fori_loop(0, rows // blk, body, 0)


def expert_down(seg, tok, gate, acts, w_down, tokens):
    rows, part = acts[0].shape
    experts, ffn, width = w_down.shape
    whole = lambda e, seg: (0, 0)
    one = pl.Buffered(1)
    return pl.pallas_call(
        functools.partial(down_kernel, len(acts)),
        out_shape=jax.ShapeDtypeStruct((tokens, width), F32),
        grid_spec=pltpu.PrefetchScalarGridSpec(
            num_scalar_prefetch=1,
            grid=(experts // EXPERT_BATCH,),
            in_specs=[pl.BlockSpec(tok.shape, whole), pl.BlockSpec(gate.shape, whole)]
            + [pl.BlockSpec((rows, part), whole, pipeline_mode=one) for _ in acts]
            + [pl.BlockSpec((EXPERT_BATCH, ffn, width), lambda e, seg: (e, 0, 0))],
            out_specs=pl.BlockSpec((tokens, width), whole, pipeline_mode=one),
            scratch_shapes=[pltpu.VMEM((rows, width), BF16)],
        ),
        compiler_params=pltpu.CompilerParams(vmem_limit_bytes=VMEM_BYTES),
        cost_estimate=cost(2 * rows * width * (ffn + tokens), 4 * rows * width),
        name='expert_down',
    )(seg, tok, gate, *acts, w_down)


def solution(mesh):
    emb_size = mesh.shape['emb']

    def local_block(hidden, norm_pre, norm_post, w_router, w_gate, w_up, w_down, choice):
        num_tok, local_width = hidden.shape
        model_width = local_width * emb_size
        experts = w_gate.shape[0]
        top_k = choice.shape[1]
        capacity = 2 * num_tok * top_k // experts
        hid_f32 = hidden.astype(F32)
        sq_pre = lax.psum(jnp.sum(hid_f32 * hid_f32, axis=1), 'emb')
        inv_pre = lax.rsqrt(sq_pre / model_width + EPS)
        tok, seg, pos = route(choice, experts, capacity)
        normed, logits = norm_logits(hidden, inv_pre, norm_pre, w_router)
        x = dispatch(tok, normed)
        logits = lax.psum(logits, 'emb')
        x, logits = lax.optimization_barrier((x, logits))
        acts = []
        for c in range(F_CHUNKS):
            z = expert_up(seg, x, w_gate, w_up, c, F_CHUNKS)
            z = lax.psum_scatter(z, 'emb', scatter_dimension=0, tiled=True)
            half = z.shape[1] // 2
            act = (jax.nn.gelu(z[:, :half].astype(F32), approximate=True) * z[:, half:].astype(F32)).astype(BF16)
            acts.append(lax.all_gather(act, 'emb', axis=0, tiled=True))
        gate = gates_of_rows(logits, choice.T, pos)
        mix = expert_down(seg, tok, gate, acts, w_down, num_tok)
        ffn_size = lax.axis_size('ffn')
        mix = lax.psum_scatter(mix, 'ffn', scatter_dimension=0, tiled=True)
        own = num_tok // ffn_size
        hid_own = lax.dynamic_slice_in_dim(hidden, lax.axis_index('ffn') * own, own, 0).astype(F32)
        sq_post = lax.psum(jnp.sum(mix * mix, axis=1), 'emb')[:, None]
        inv_post = lax.rsqrt(sq_post / model_width + EPS)
        out = (hid_own + mix * inv_post * norm_post.astype(F32)).astype(BF16)
        return lax.all_gather(out, 'ffn', axis=0, tiled=True)

    in_specs = (P('dp', 'emb'), P('emb'), P('emb'), P('emb', None), P(None, 'emb', 'ffn'), P(None, 'emb', 'ffn'), P(None, 'ffn', 'emb'), P('dp', None))
    return jax.shard_map(local_block, mesh=mesh, in_specs=in_specs, out_specs=P('dp', 'emb'), check_vma=False)
```

```python
import functools

import jax
import jax.numpy as jnp
from jax import lax
from jax.experimental import pallas as pl
from jax.experimental.pallas import tpu as pltpu
from jax.sharding import PartitionSpec as P

EPS = 1e-5
LANE = 128
ROW_BLOCK = 272
EXPERT_BATCH = 4
VMEM_BYTES = 60 * 1024 * 1024
F32 = jnp.float32
BF16 = jnp.bfloat16
MESH = pl.DeviceIdType.MESH


def cost(flops, nbytes):
    return pl.CostEstimate(flops=int(flops), bytes_accessed=int(nbytes), transcendentals=0)


def greet(peers):
    barrier = pltpu.get_barrier_semaphore()
    count = 0
    for peer in peers:
        pl.semaphore_signal(barrier, inc=1, device_id=peer, device_id_type=MESH)
        count += 1
    pl.semaphore_wait(barrier, count)


def onehot_pieces(pos_row, rows_hi):
    tokens = pos_row.shape[1]
    hi = jnp.floor(pos_row * (1.0 / LANE))
    lo = pos_row - hi * LANE
    hi_iota = lax.broadcasted_iota(jnp.int32, (rows_hi, tokens), 0).astype(F32)
    lo_iota = lax.broadcasted_iota(jnp.int32, (LANE, tokens), 0).astype(F32)
    return hi == hi_iota, lo == lo_iota


def route_kernel(capacity, experts, choice_ref, tok_ref, seg_ref, pos_ref):
    top_k, tokens = choice_ref.shape
    rows_hi = tok_ref.shape[0]
    rows = rows_hi * LANE
    blk = 256
    e_iota = lax.broadcasted_iota(jnp.int32, (experts, tokens), 0)
    assigned = jnp.zeros((experts, tokens), F32)
    for k in range(top_k):
        assigned += jnp.where(choice_ref[k:k + 1, :] == e_iota, 1.0, 0.0)
    r_i = lax.broadcasted_iota(jnp.int32, (blk, blk), 0)
    c_i = lax.broadcasted_iota(jnp.int32, (blk, blk), 1)
    tri = jnp.where(r_i < c_i, 1.0, 0.0).astype(BF16)
    carry = jnp.zeros((experts, 1), F32)
    before = []
    for b in range(tokens // blk):
        part = assigned[:, b * blk:(b + 1) * blk]
        within = jnp.dot(part.astype(BF16), tri, preferred_element_type=F32)
        before.append(within + carry)
        carry = carry + jnp.sum(part, axis=1, keepdims=True)
    before = jnp.concatenate(before, axis=1)
    kept = jnp.broadcast_to(jnp.minimum(carry, float(capacity)), (experts, LANE))
    kept_hi = jnp.floor(kept * (1.0 / 16.0))
    kept_lo = kept - kept_hi * 16.0
    er = lax.broadcasted_iota(jnp.int32, (experts, experts), 0)
    ec = lax.broadcasted_iota(jnp.int32, (experts, experts), 1)
    low = jnp.where(ec < er, 1.0, 0.0).astype(BF16)
    start = 16.0 * jnp.dot(low, kept_hi.astype(BF16), preferred_element_type=F32)
    start = start + jnp.dot(low, kept_lo.astype(BF16), preferred_element_type=F32)
    end = start + kept
    fill = jnp.zeros((LANE - experts, LANE), F32)
    start_t = jnp.transpose(jnp.concatenate([start, fill], axis=0))
    end_t = jnp.transpose(jnp.concatenate([end, fill], axis=0))
    seg_ref[0:1, :] = start_t[0:1, :].astype(jnp.int32)
    lane = lax.broadcasted_iota(jnp.int32, (1, LANE), 1)
    seg_ref[1:2, :] = jnp.where(lane == experts - 1, rows, end_t[0:1, :].astype(jnp.int32))
    value = jnp.where(before < capacity, before + start[:, 0:1], float(rows))
    t_val = lax.broadcasted_iota(jnp.int32, (1, tokens), 1) + 1
    t_hi = (t_val // 16).astype(F32)
    t_lo = (t_val % 16).astype(F32)
    acc = jnp.zeros((rows_hi, 2 * LANE), F32)
    for k in range(top_k):
        hit = choice_ref[k:k + 1, :] == e_iota
        pos = jnp.sum(jnp.where(hit, value, 0.0), axis=0, keepdims=True)
        pos_ref[k:k + 1, :] = pos
        is_hi, is_lo = onehot_pieces(pos, rows_hi)
        left = jnp.where(is_hi, 1.0, 0.0).astype(BF16)
        right = jnp.concatenate([jnp.where(is_lo, t_hi, 0.0), jnp.where(is_lo, t_lo, 0.0)], axis=0).astype(BF16)
        acc += lax.dot_general(left, right, (((1,), (1,)), ((), ())), preferred_element_type=F32)
    tok_ref[...] = (16.0 * acc[:, :LANE] + acc[:, LANE:]).astype(jnp.int32) - 1


def route(choice, experts, capacity):
    tokens, top_k = choice.shape
    rows_hi = tokens * top_k // LANE
    return pl.pallas_call(
        functools.partial(route_kernel, capacity, experts),
        out_shape=(
            jax.ShapeDtypeStruct((rows_hi, LANE), jnp.int32),
            jax.ShapeDtypeStruct((2, LANE), jnp.int32),
            jax.ShapeDtypeStruct((top_k, tokens), F32),
        ),
        compiler_params=pltpu.CompilerParams(vmem_limit_bytes=VMEM_BYTES),
        cost_estimate=cost(10e9, 1e5),
        name='route',
    )(choice.T)


def norm_kernel(hid_ref, inv_ref, pre_ref, wr_ref, b_ref, logit_ref):
    width = hid_ref.shape[1]
    for i in range(inv_ref.shape[0]):
        col = jnp.concatenate([column_of(inv_ref[i:i + 1, :])] * (width // LANE), axis=1)
        part = slice(i * LANE, (i + 1) * LANE)
        b_ref[part, :] = (hid_ref[part, :].astype(F32) * col * pre_ref[...].astype(F32)).astype(BF16)
    b = b_ref[...]
    logit_ref[...] = lax.dot_general(wr_ref[...], b, (((0,), (1,)), ((), ())), preferred_element_type=F32)


def norm_logits(hidden, inv_pre, norm_pre, w_router):
    tokens, width = hidden.shape
    experts = w_router.shape[1]
    return pl.pallas_call(
        norm_kernel,
        out_shape=(
            jax.ShapeDtypeStruct((tokens, width), BF16),
            jax.ShapeDtypeStruct((experts, tokens), F32),
        ),
        compiler_params=pltpu.CompilerParams(vmem_limit_bytes=VMEM_BYTES),
        cost_estimate=cost(5e9, 3e6),
        name='norm_logits',
    )(hidden, inv_pre.reshape(tokens // LANE, LANE), norm_pre.reshape(1, width), w_router)


def column_of(row):
    return jnp.transpose(jnp.broadcast_to(row, (LANE, LANE)))


def dispatch_kernel(tok_ref, b_ref, x_ref):
    i = pl.program_id(0)
    tokens = b_ref.shape[0]
    rows = x_ref.shape[0]
    lane = lax.broadcasted_iota(jnp.int32, (LANE, LANE), 1)
    strips = []
    for q in range(rows // LANE):
        col = column_of(tok_ref[pl.ds(i * (rows // LANE) + q, 1), :])
        strips.append(jnp.concatenate(
            [jnp.where(col == lane + j * LANE, 1.0, 0.0).astype(BF16) for j in range(tokens // LANE)], axis=1))
    pick = jnp.concatenate(strips, axis=0)
    x_ref[...] = jnp.dot(pick, b_ref[...], preferred_element_type=F32).astype(BF16)


def dispatch(tok, b):
    tokens, width = b.shape
    rows = tok.size
    blk = 512
    return pl.pallas_call(
        dispatch_kernel,
        out_shape=jax.ShapeDtypeStruct((rows, width), BF16),
        grid=(rows // blk,),
        in_specs=[
            pl.BlockSpec(tok.shape, lambda i: (0, 0)),
            pl.BlockSpec((tokens, width), lambda i: (0, 0)),
        ],
        out_specs=pl.BlockSpec((blk, width), lambda i: (i, 0)),
        compiler_params=pltpu.CompilerParams(vmem_limit_bytes=VMEM_BYTES),
        cost_estimate=cost(2 * rows * tokens * width, rows * width * 2),
        name='dispatch',
    )(tok, b)


def grouped(seg_ref, step, in_refs, weights, out_ref):
    total = out_ref.shape[0]
    batch = len(weights)

    def block(e, w, offset):
        s = seg_ref[0, e]
        r0 = pl.multiple_of(jnp.minimum((s // 16) * 16 + offset, total - ROW_BLOCK), 16)
        parts = [r[pl.ds(r0, ROW_BLOCK), :] for r in in_refs]
        src = parts[0] if len(parts) == 1 else jnp.concatenate(parts, axis=1)
        new = jnp.dot(src, w(), preferred_element_type=F32).astype(BF16)
        return s, r0, new

    def put(s, r0, new):
        row = r0 + lax.broadcasted_iota(jnp.int32, new.shape, 0)
        out_ref[pl.ds(r0, ROW_BLOCK), :] = jnp.where(row >= s, new, out_ref[pl.ds(r0, ROW_BLOCK), :])

    long = jnp.bool_(False)
    for q in range(batch):
        e = step * batch + q
        long = jnp.logical_or(long, seg_ref[1, e] - (seg_ref[0, e] // 16) * 16 > ROW_BLOCK)

    @pl.when(jnp.logical_not(long))
    def short_segments():
        for item in [block(step * batch + q, weights[q], 0) for q in range(batch)]:
            put(*item)

    @pl.when(long)
    def long_segments():
        for q in range(batch):
            e = step * batch + q
            count = (seg_ref[1, e] - (seg_ref[0, e] // 16) * 16 + ROW_BLOCK - 1) // ROW_BLOCK

            def body(j, carry):
                put(*block(e, weights[q], j * ROW_BLOCK))
                return carry

            lax.fori_loop(0, count, body, 0)


def up_kernel(seg_ref, x_ref, wg_ref, wu_ref, z_ref):
    pick = lambda q: lambda: jnp.concatenate([wg_ref[q], wu_ref[q]], axis=1)
    grouped(seg_ref, pl.program_id(0), [x_ref], [pick(q) for q in range(wg_ref.shape[0])], z_ref)


def expert_up(seg, x, w_gate, w_up, chunk, chunks):
    rows, width = x.shape
    experts, _, ffn = w_gate.shape
    part = ffn // chunks
    w_spec = pl.BlockSpec((EXPERT_BATCH, width, part), lambda e, seg: (e, 0, chunk))
    return pl.pallas_call(
        up_kernel,
        out_shape=jax.ShapeDtypeStruct((rows, 2 * part), BF16),
        grid_spec=pltpu.PrefetchScalarGridSpec(
            num_scalar_prefetch=1,
            grid=(experts // EXPERT_BATCH,),
            in_specs=[pl.BlockSpec((rows, width), lambda e, seg: (0, 0), pipeline_mode=pl.Buffered(1)), w_spec, w_spec],
            out_specs=pl.BlockSpec((rows, 2 * part), lambda e, seg: (0, 0), pipeline_mode=pl.Buffered(1)),
        ),
        compiler_params=pltpu.CompilerParams(vmem_limit_bytes=VMEM_BYTES),
        cost_estimate=cost(8 * rows * width * part, 4 * rows * width),
        name='expert_up',
    )(seg, x, w_gate, w_up)


def exchange_kernel(emb_size, subs, z_ref, g_ref, mine, theirs, ring, load, send_p, recv_p, send_r, recv_r,
                    send_a, recv_a, send_d, recv_d):
    chips = emb_size // 2
    last = chips - 1
    me = lax.axis_index('emb')
    chip, core = me // 2, lax.rem(me, 2)
    partner = {'emb': chip * 2 + 1 - core}
    ways = [{'emb': lax.rem(me + 2, emb_size)}, {'emb': lax.rem(me + emb_size - 2, emb_size)}]
    own = z_ref.shape[0] // emb_size
    half = own // 2
    sub = half // subs
    ffn = g_ref.shape[1]
    greet([partner] + ways)

    def around(c):
        return lax.rem(c + 2 * chips, chips)

    def target(d, step):
        return around(chip - 1 - step if d == 0 else chip + 1 + step)

    def rows(c, parity, d, u, size):
        return pl.ds(pl.multiple_of((c * 2 + parity) * own + d * half + u * sub, sub), size)

    order = [(step, u, d) for step in range(chips) for u in range(subs) for d in range(2)]
    loads, passed, sums = {}, {}, {}
    for step, u, d in order:
        c = target(d, step)
        copy = pltpu.make_async_remote_copy(
            src_ref=z_ref.at[rows(c, 1 - core, d, u, sub), :], dst_ref=theirs.at[step, d, u],
            send_sem=send_p.at[step, d, u], recv_sem=recv_p.at[step, d, u],
            device_id=partner, device_id_type=MESH)
        copy.start()
        passed[step, d, u] = copy
        copy = pltpu.make_async_copy(z_ref.at[rows(c, core, d, u, sub), :], mine.at[step, d, u], load.at[step, d, u])
        copy.start()
        loads[step, d, u] = copy

    spread = {}

    def scatter(d, way, step, c, u):
        at = rows(c, core, d, u, sub)
        copy = pltpu.make_async_remote_copy(
            src_ref=g_ref.at[at, :], dst_ref=g_ref.at[at, :],
            send_sem=send_a.at[way, step, d, u], recv_sem=recv_a.at[way, step, d, u],
            device_id=ways[way], device_id_type=MESH)
        copy.start()
        spread[way, step, d, u] = copy

    across = {}

    def share(d, slot, c, u):
        at = rows(c, core, d, u, sub)
        copy = pltpu.make_async_remote_copy(
            src_ref=g_ref.at[at, :], dst_ref=g_ref.at[at, :],
            send_sem=send_d.at[slot, d, u], recv_sem=recv_d.at[slot, d, u],
            device_id=partner, device_id_type=MESH)
        copy.start()
        across[slot, d, u] = copy

    def sends(way, step, d):
        if step < (chips - 1) // 2:
            return True
        return step == (chips - 1) // 2 and chips % 2 == 0 and way == d

    piece = 32
    for step, u, d in order:
        loads[step, d, u].wait()
        passed[step, d, u].wait_recv()
        if step >= 1:
            sums[step - 1, d, u].wait_recv()
        if step < last:
            def add(i, carry):
                at = pl.ds(pl.multiple_of(i * piece, piece), piece)
                v = mine[step, d, u, at, :].astype(F32) + theirs[step, d, u, at, :].astype(F32)
                if step >= 1:
                    v = v + ring[step - 1, d, u, at, :].astype(F32)
                mine[step, d, u, at, :] = v.astype(BF16)
                return carry

            lax.fori_loop(0, sub // piece, add, 0)
            copy = pltpu.make_async_remote_copy(
                src_ref=mine.at[step, d, u], dst_ref=ring.at[step, d, u],
                send_sem=send_r.at[step, d, u], recv_sem=recv_r.at[step, d, u],
                device_id=ways[d], device_id_type=MESH)
            copy.start()
            sums[step, d, u] = copy
        else:
            def act(i, carry):
                at = pl.ds(pl.multiple_of(i * piece, piece), piece)
                v = mine[step, d, u, at, :].astype(F32) + theirs[step, d, u, at, :].astype(F32)
                v = (v + ring[step - 1, d, u, at, :].astype(F32)).astype(BF16).astype(F32)
                v = jax.nn.gelu(v[:, :ffn], approximate=True) * v[:, ffn:]
                out = pl.ds(pl.multiple_of((chip * 2 + core) * own + d * half + u * sub + i * piece, piece), piece)
                g_ref[out, :] = v.astype(BF16)
                return carry

            lax.fori_loop(0, sub // piece, act, 0)
            for way in range(2):
                if sends(way, 0, d):
                    scatter(d, way, 0, chip, u)
            share(d, 0, chip, u)
    slot = 0
    for step in range(chips // 2):
        for u in range(subs):
            for way in range(2):
                for d in range(2):
                    if sends(way, step, d):
                        spread[way, step, d, u].wait_recv()
                        c = around(chip - 1 - step if way == 0 else chip + 1 + step)
                        if sends(way, step + 1, d):
                            scatter(d, way, step + 1, c, u)
                        full = sends(0, step, d) and sends(1, step, d)
                        share(d, 1 + 2 * step + (way if full else 0), c, u)
    for copy in across.values():
        copy.wait_recv()
    for group in (passed, sums, spread, across):
        for copy in group.values():
            copy.wait_send()


def exchange(z, emb_size):
    rows, both = z.shape
    chips = emb_size // 2
    own = rows // emb_size
    subs = 4
    sub = own // (2 * subs)
    dma = pltpu.SemaphoreType.DMA
    part = (chips, 2, subs)
    hop = (chips - 1, 2, subs)
    fan = (2, max(chips // 2, 1), 2, subs)
    return pl.pallas_call(
        functools.partial(exchange_kernel, emb_size, subs),
        out_shape=jax.ShapeDtypeStruct((rows, both // 2), BF16),
        in_specs=[pl.BlockSpec(memory_space=pl.ANY)],
        out_specs=pl.BlockSpec(memory_space=pltpu.VMEM),
        scratch_shapes=[
            pltpu.VMEM(part + (sub, both), BF16),
            pltpu.VMEM(part + (sub, both), BF16),
            pltpu.VMEM(hop + (sub, both), BF16),
            dma(part), dma(part), dma(part), dma(hop), dma(hop), dma(fan), dma(fan), dma(part), dma(part),
        ],
        compiler_params=pltpu.CompilerParams(collective_id=2, has_side_effects=True, vmem_limit_bytes=VMEM_BYTES),
        cost_estimate=cost(100e9, 4 * rows * both),
        name='exchange',
    )(z)


def gate_kernel(emb_size, logit_ref, choice_ref, pos_ref, gate_ref, got, gates, send_a, recv_a, send_b, recv_b):
    experts, tokens = logit_ref.shape
    top_k = choice_ref.shape[0]
    rows_hi = gate_ref.shape[0]
    own = tokens // emb_size
    me = lax.axis_index('emb')
    greet({'emb': lax.rem(me + j, emb_size)} for j in range(1, emb_size))

    def columns(who):
        return pl.ds(pl.multiple_of(who * own, own), own)

    parts = []
    for j in range(1, emb_size):
        peer = lax.rem(me + j, emb_size)
        parts.append(pltpu.make_async_remote_copy(
            src_ref=logit_ref.at[:, columns(peer)], dst_ref=got.at[j - 1],
            send_sem=send_a.at[j - 1], recv_sem=recv_a.at[j - 1],
            device_id={'emb': peer}, device_id_type=MESH))
        parts[-1].start()
    logits = logit_ref[:, columns(me)]
    for j in range(1, emb_size):
        parts[j - 1].wait_recv()
        logits = logits + got[j - 1]
    grown = jnp.exp(logits - jnp.max(logits, axis=0, keepdims=True))
    prob = grown / jnp.sum(grown, axis=0, keepdims=True)
    e_iota = lax.broadcasted_iota(jnp.int32, (experts, own), 0)
    mine = choice_ref[:, columns(me)]
    for k in range(top_k):
        gates[k:k + 1, columns(me)] = jnp.sum(jnp.where(mine[k:k + 1, :] == e_iota, prob, 0.0), axis=0, keepdims=True)
    picked = []
    for j in range(1, emb_size):
        picked.append(pltpu.make_async_remote_copy(
            src_ref=gates.at[:, columns(me)], dst_ref=gates.at[:, columns(me)],
            send_sem=send_b.at[j - 1], recv_sem=recv_b.at[j - 1],
            device_id={'emb': lax.rem(me + j, emb_size)}, device_id_type=MESH))
        picked[-1].start()
    for copy in parts:
        copy.wait_send()
    for copy in picked:
        copy.wait()
    acc = jnp.zeros((rows_hi, 3 * LANE), F32)
    for k in range(top_k):
        is_hi, is_lo = onehot_pieces(pos_ref[k:k + 1, :], rows_hi)
        left = jnp.where(is_hi, 1.0, 0.0).astype(BF16)
        pieces = []
        rest = gates[k:k + 1, :]
        for _ in range(3):
            piece = rest.astype(BF16).astype(F32)
            rest = rest - piece
            pieces.append(jnp.where(is_lo, piece, 0.0).astype(BF16))
        right = jnp.concatenate(pieces, axis=0)
        acc += lax.dot_general(left, right, (((1,), (1,)), ((), ())), preferred_element_type=F32)
    gate_ref[...] = acc[:, :LANE] + acc[:, LANE:2 * LANE] + acc[:, 2 * LANE:]


def gates_of_rows(logits, choice_t, pos, emb_size):
    top_k, tokens = choice_t.shape
    experts = logits.shape[0]
    rows_hi = tokens * top_k // LANE
    others = emb_size - 1
    dma = pltpu.SemaphoreType.DMA((others,))
    vmem = pl.BlockSpec(memory_space=pltpu.VMEM)
    return pl.pallas_call(
        functools.partial(gate_kernel, emb_size),
        out_shape=jax.ShapeDtypeStruct((rows_hi, LANE), F32),
        in_specs=[vmem, vmem, vmem],
        out_specs=vmem,
        scratch_shapes=[
            pltpu.VMEM((others, experts, tokens // emb_size), F32),
            pltpu.VMEM((top_k, tokens), F32),
            dma, dma, dma, dma,
        ],
        compiler_params=pltpu.CompilerParams(collective_id=0, has_side_effects=True),
        cost_estimate=cost(15e9, 1e6),
        name='gates',
    )(logits, choice_t, pos)


def finish_kernel(ffn_size, emb_size, model_width, mix_ref, hid_ref, post_ref, out_ref, got, total, squares,
                  send_a, recv_a, send_b, recv_b, send_c, recv_c):
    tokens, width = mix_ref.shape
    own = tokens // ffn_size
    half = width // 2
    subs = got.shape[2]
    sub = own // subs
    me = lax.axis_index('ffn')
    emb = lax.axis_index('emb')
    right, left = lax.rem(me + 1, ffn_size), lax.rem(me + ffn_size - 1, ffn_size)
    peers = [{'ffn': right}, {'ffn': left}]
    greet(peers + [{'emb': lax.rem(emb + j, emb_size)} for j in range(1, emb_size)])

    def mix_part(d, step, u):
        chunk = me - 1 - step if d == 0 else me + 1 + step
        chunk = lax.rem(chunk + ffn_size * 2, ffn_size)
        row = pl.multiple_of(chunk * own + u * sub, sub)
        return mix_ref.at[pl.ds(row, sub), d * half:(d + 1) * half]

    sums = {}

    def send(d, step, u):
        copy = pltpu.make_async_remote_copy(
            src_ref=mix_part(d, 0, u) if step == 0 else got.at[d, step - 1, u], dst_ref=got.at[d, step, u],
            send_sem=send_a.at[d, step, u], recv_sem=recv_a.at[d, step, u],
            device_id=peers[d], device_id_type=MESH)
        copy.start()
        sums[d, step, u] = copy

    for u in range(subs):
        for d in range(2):
            send(d, 0, u)
    for step in range(1, ffn_size):
        for u in range(subs):
            for d in range(2):
                sums[d, step - 1, u].wait_recv()
                if step < ffn_size - 1:
                    got[d, step - 1, u] = got[d, step - 1, u] + mix_part(d, step, u)[...]
                    send(d, step, u)
                else:
                    total[u * sub:(u + 1) * sub, d * half:(d + 1) * half] = got[d, step - 1, u] + mix_part(d, step, u)[...]
    for i in range(own // LANE):
        part = total[i * LANE:(i + 1) * LANE, :]
        part = part * part
        lanes = part[:, :LANE]
        for j in range(1, width // LANE):
            lanes = lanes + part[:, j * LANE:(j + 1) * LANE]
        squares[emb_size - 1, i:i + 1, :] = jnp.sum(jnp.transpose(lanes), axis=0, keepdims=True)
    shares = []
    for j in range(1, emb_size):
        shares.append(pltpu.make_async_remote_copy(
            src_ref=squares.at[emb_size - 1], dst_ref=squares.at[j - 1],
            send_sem=send_b.at[j - 1], recv_sem=recv_b.at[j - 1],
            device_id={'emb': lax.rem(emb + j, emb_size)}, device_id_type=MESH))
        shares[-1].start()
    for copy in shares:
        copy.wait_recv()
    whole = squares[emb_size - 1]
    for j in range(emb_size - 1):
        whole = whole + squares[j]
    inv = lax.rsqrt(whole / model_width + EPS)
    post = post_ref[...].astype(F32)

    def rows(chunk, start, size):
        chunk = lax.rem(chunk + ffn_size * 2, ffn_size)
        return pl.ds(pl.multiple_of(chunk * own + start, size), size)

    for i in range(own // LANE):
        col = jnp.concatenate([column_of(inv[i:i + 1, :])] * (width // LANE), axis=1)
        at = rows(me, i * LANE, LANE)
        out_ref[at, :] = (hid_ref[at, :].astype(F32) + total[i * LANE:(i + 1) * LANE, :] * col * post).astype(BF16)
    spread = []
    for step in range(ffn_size // 2):
        if step >= 1:
            for copy in spread[-2:]:
                copy.wait_recv()
        last = step == (ffn_size - 1) // 2
        for d in range(2):
            chunk = me - step if d == 0 else me + step
            at = rows(chunk, d * own // 2, own // 2) if last else rows(chunk, 0, own)
            spread.append(pltpu.make_async_remote_copy(
                src_ref=out_ref.at[at, :], dst_ref=out_ref.at[at, :],
                send_sem=send_c.at[d, step], recv_sem=recv_c.at[d, step],
                device_id=peers[d], device_id_type=MESH))
            spread[-1].start()
    for copy in spread[-2:]:
        copy.wait_recv()
    for copy in list(sums.values()) + shares + spread:
        copy.wait_send()


def finish(mix, hidden, norm_post, ffn_size, emb_size):
    tokens, width = mix.shape
    own = tokens // ffn_size
    subs = 2 if own % 256 == 0 else 1
    vmem = pl.BlockSpec(memory_space=pltpu.VMEM)
    dma = pltpu.SemaphoreType.DMA
    return pl.pallas_call(
        functools.partial(finish_kernel, ffn_size, emb_size, width * emb_size),
        out_shape=jax.ShapeDtypeStruct((tokens, width), BF16),
        in_specs=[vmem, vmem, vmem],
        out_specs=vmem,
        scratch_shapes=[
            pltpu.VMEM((2, ffn_size - 1, subs, own // subs, width // 2), F32),
            pltpu.VMEM((own, width), F32),
            pltpu.VMEM((emb_size, own // LANE, LANE), F32),
            dma((2, ffn_size - 1, subs)), dma((2, ffn_size - 1, subs)),
            dma((emb_size - 1,)), dma((emb_size - 1,)),
            dma((2, ffn_size // 2)), dma((2, ffn_size // 2)),
        ],
        compiler_params=pltpu.CompilerParams(collective_id=1, has_side_effects=True),
        cost_estimate=cost(30e9, 8e6),
        name='finish',
    )(mix, hidden, norm_post.reshape(1, width))


def down_kernel(chunks, seg_ref, tok_ref, gate_ref, *refs):
    g_refs = refs[:chunks]
    w_ref, m_ref, y_ref = refs[chunks:]
    tokens, width = m_ref.shape
    rows = y_ref.shape[0]
    pick = lambda q: lambda: w_ref[q]
    grouped(seg_ref, pl.program_id(0), g_refs, [pick(q) for q in range(w_ref.shape[0])], y_ref)

    @pl.when(pl.program_id(0) == pl.num_programs(0) - 1)
    def combine():
        blk = 512
        t_iota = lax.broadcasted_iota(jnp.int32, (tokens, LANE), 0)
        m_ref[...] = jnp.zeros_like(m_ref)

        def body(i, carry):
            scaled, picks = [], []
            for q in range(blk // LANE):
                hi = i * (blk // LANE) + q
                col = column_of(gate_ref[pl.ds(hi, 1), :])
                col = jnp.concatenate([col] * (width // LANE), axis=1)
                r0 = pl.multiple_of(hi * LANE, LANE)
                scaled.append((y_ref[pl.ds(r0, LANE), :].astype(F32) * col).astype(BF16))
                picks.append(jnp.where(t_iota == tok_ref[pl.ds(hi, 1), :], 1.0, 0.0).astype(BF16))
            u = jnp.concatenate(scaled, axis=0)
            pick = jnp.concatenate(picks, axis=1)
            m_ref[...] += jnp.dot(pick, u, preferred_element_type=F32)
            return carry

        lax.fori_loop(0, rows // blk, body, 0)


def expert_down(seg, tok, gate, acts, w_down, tokens):
    rows, part = acts[0].shape
    experts, ffn, width = w_down.shape
    whole = lambda e, seg: (0, 0)
    one = pl.Buffered(1)
    return pl.pallas_call(
        functools.partial(down_kernel, len(acts)),
        out_shape=jax.ShapeDtypeStruct((tokens, width), F32),
        grid_spec=pltpu.PrefetchScalarGridSpec(
            num_scalar_prefetch=1,
            grid=(experts // EXPERT_BATCH,),
            in_specs=[pl.BlockSpec(tok.shape, whole), pl.BlockSpec(gate.shape, whole)]
            + [pl.BlockSpec((rows, part), whole, pipeline_mode=one) for _ in acts]
            + [pl.BlockSpec((EXPERT_BATCH, ffn, width), lambda e, seg: (e, 0, 0))],
            out_specs=pl.BlockSpec((tokens, width), whole, pipeline_mode=one),
            scratch_shapes=[pltpu.VMEM((rows, width), BF16)],
        ),
        compiler_params=pltpu.CompilerParams(vmem_limit_bytes=VMEM_BYTES),
        cost_estimate=cost(2 * rows * width * (ffn + tokens), 4 * rows * width),
        name='expert_down',
    )(seg, tok, gate, *acts, w_down)


def solution(mesh):
    emb_size = mesh.shape['emb']
    ffn_size = mesh.shape['ffn']

    def local_block(hidden, norm_pre, norm_post, w_router, w_gate, w_up, w_down, choice):
        num_tok, local_width = hidden.shape
        model_width = local_width * emb_size
        experts = w_gate.shape[0]
        top_k = choice.shape[1]
        capacity = 2 * num_tok * top_k // experts
        hid_f32 = hidden.astype(F32)
        sq_pre = lax.psum(jnp.sum(hid_f32 * hid_f32, axis=1), 'emb')
        inv_pre = lax.rsqrt(sq_pre / model_width + EPS)
        tok, seg, pos = route(choice, experts, capacity)
        normed, logits = norm_logits(hidden, inv_pre, norm_pre, w_router)
        x = dispatch(tok, normed)
        z = expert_up(seg, x, w_gate, w_up, 0, 1)
        act = exchange(z, emb_size)
        gate = gates_of_rows(logits, choice.T, pos, emb_size)
        mix = expert_down(seg, tok, gate, [act], w_down, num_tok)
        return finish(mix, hidden, norm_post, ffn_size, emb_size)

    in_specs = (P('dp', 'emb'), P('emb'), P('emb'), P('emb', None), P(None, 'emb', 'ffn'), P(None, 'emb', 'ffn'), P(None, 'ffn', 'emb'), P('dp', None))
    return jax.shard_map(local_block, mesh=mesh, in_specs=in_specs, out_specs=P('dp', 'emb'), check_vma=False)
```

```python
import functools

import jax
import jax.numpy as jnp
from jax import lax
from jax.experimental import pallas as pl
from jax.experimental.pallas import tpu as pltpu
from jax.sharding import PartitionSpec as P

EPS = 1e-5
LANE = 128
ROW_BLOCK = 272
EXPERT_BATCH = 8
VMEM_BYTES = 60 * 1024 * 1024
F32 = jnp.float32
BF16 = jnp.bfloat16
MESH = pl.DeviceIdType.MESH


def cost(flops, nbytes):
    return pl.CostEstimate(flops=int(flops), bytes_accessed=int(nbytes), transcendentals=0)


def greet(peers):
    barrier = pltpu.get_barrier_semaphore()
    count = 0
    for peer in peers:
        pl.semaphore_signal(barrier, inc=1, device_id=peer, device_id_type=MESH)
        count += 1
    pl.semaphore_wait(barrier, count)


def onehot_pieces(pos_row, rows_hi):
    tokens = pos_row.shape[1]
    hi = jnp.floor(pos_row * (1.0 / LANE))
    lo = pos_row - hi * LANE
    hi_iota = lax.broadcasted_iota(jnp.int32, (rows_hi, tokens), 0).astype(F32)
    lo_iota = lax.broadcasted_iota(jnp.int32, (LANE, tokens), 0).astype(F32)
    return hi == hi_iota, lo == lo_iota


def route_rows(capacity, experts, choice_ref, tok_ref, seg_ref, pos_ref):
    top_k, tokens = choice_ref.shape
    rows_hi = tok_ref.shape[0]
    rows = rows_hi * LANE
    blk = 256
    e_iota = lax.broadcasted_iota(jnp.int32, (experts, tokens), 0)
    assigned = jnp.zeros((experts, tokens), F32)
    for k in range(top_k):
        assigned += jnp.where(choice_ref[k:k + 1, :] == e_iota, 1.0, 0.0)
    r_i = lax.broadcasted_iota(jnp.int32, (blk, blk), 0)
    c_i = lax.broadcasted_iota(jnp.int32, (blk, blk), 1)
    tri = jnp.where(r_i < c_i, 1.0, 0.0).astype(BF16)
    carry = jnp.zeros((experts, 1), F32)
    before = []
    for b in range(tokens // blk):
        part = assigned[:, b * blk:(b + 1) * blk]
        within = jnp.dot(part.astype(BF16), tri, preferred_element_type=F32)
        before.append(within + carry)
        carry = carry + jnp.sum(part, axis=1, keepdims=True)
    before = jnp.concatenate(before, axis=1)
    kept = jnp.broadcast_to(jnp.minimum(carry, float(capacity)), (experts, LANE))
    kept_hi = jnp.floor(kept * (1.0 / 16.0))
    kept_lo = kept - kept_hi * 16.0
    er = lax.broadcasted_iota(jnp.int32, (experts, experts), 0)
    ec = lax.broadcasted_iota(jnp.int32, (experts, experts), 1)
    low = jnp.where(ec < er, 1.0, 0.0).astype(BF16)
    start = 16.0 * jnp.dot(low, kept_hi.astype(BF16), preferred_element_type=F32)
    start = start + jnp.dot(low, kept_lo.astype(BF16), preferred_element_type=F32)
    end = start + kept
    fill = jnp.zeros((LANE - experts, LANE), F32)
    start_t = jnp.transpose(jnp.concatenate([start, fill], axis=0))
    end_t = jnp.transpose(jnp.concatenate([end, fill], axis=0))
    seg_ref[0:1, :] = start_t[0:1, :].astype(jnp.int32)
    lane = lax.broadcasted_iota(jnp.int32, (1, LANE), 1)
    seg_ref[1:2, :] = jnp.where(lane == experts - 1, rows, end_t[0:1, :].astype(jnp.int32))
    value = jnp.where(before < capacity, before + start[:, 0:1], float(rows))
    t_val = lax.broadcasted_iota(jnp.int32, (1, tokens), 1) + 1
    t_hi = (t_val // 16).astype(F32)
    t_lo = (t_val % 16).astype(F32)
    acc = jnp.zeros((rows_hi, 2 * LANE), F32)
    for k in range(top_k):
        hit = choice_ref[k:k + 1, :] == e_iota
        pos = jnp.sum(jnp.where(hit, value, 0.0), axis=0, keepdims=True)
        pos_ref[k:k + 1, :] = pos
        is_hi, is_lo = onehot_pieces(pos, rows_hi)
        left = jnp.where(is_hi, 1.0, 0.0).astype(BF16)
        right = jnp.concatenate([jnp.where(is_lo, t_hi, 0.0), jnp.where(is_lo, t_lo, 0.0)], axis=0).astype(BF16)
        acc += lax.dot_general(left, right, (((1,), (1,)), ((), ())), preferred_element_type=F32)
    tok_ref[...] = (16.0 * acc[:, :LANE] + acc[:, LANE:]).astype(jnp.int32) - 1


def square_rows(block):
    block = block * block
    lanes = block[:, :LANE]
    for j in range(1, block.shape[1] // LANE):
        lanes = lanes + block[:, j * LANE:(j + 1) * LANE]
    return jnp.sum(jnp.transpose(lanes), axis=0, keepdims=True)


def share_squares(squares, emb_size, send, recv):
    me = lax.axis_index('emb')
    copies = []
    for j in range(1, emb_size):
        copies.append(pltpu.make_async_remote_copy(
            src_ref=squares.at[emb_size - 1], dst_ref=squares.at[j - 1],
            send_sem=send.at[j - 1], recv_sem=recv.at[j - 1],
            device_id={'emb': lax.rem(me + j, emb_size)}, device_id_type=MESH))
        copies[-1].start()
    return copies


def inverse_rms(squares, emb_size, model_width):
    whole = squares[emb_size - 1]
    for j in range(emb_size - 1):
        whole = whole + squares[j]
    return lax.rsqrt(whole / model_width + EPS)


def prepare_kernel(capacity, emb_size, model_width, choice_ref, hid_ref, pre_ref, wr_ref,
                   tok_ref, seg_ref, pos_ref, b_ref, logit_ref, squares, send, recv):
    tokens, width = hid_ref.shape
    me = lax.axis_index('emb')
    greet({'emb': lax.rem(me + j, emb_size)} for j in range(1, emb_size))
    for i in range(tokens // LANE):
        squares[emb_size - 1, i:i + 1, :] = square_rows(hid_ref[i * LANE:(i + 1) * LANE, :].astype(F32))
    copies = share_squares(squares, emb_size, send, recv)
    route_rows(capacity, wr_ref.shape[1], choice_ref, tok_ref, seg_ref, pos_ref)
    for copy in copies:
        copy.wait_recv()
    inv = inverse_rms(squares, emb_size, model_width)
    pre = pre_ref[...].astype(F32)
    for i in range(tokens // LANE):
        col = jnp.concatenate([column_of(inv[i:i + 1, :])] * (width // LANE), axis=1)
        part = slice(i * LANE, (i + 1) * LANE)
        b_ref[part, :] = (hid_ref[part, :].astype(F32) * col * pre).astype(BF16)
    logit_ref[...] = lax.dot_general(wr_ref[...], b_ref[...], (((0,), (1,)), ((), ())), preferred_element_type=F32)
    for copy in copies:
        copy.wait_send()


def prepare(choice_t, hidden, norm_pre, w_router, capacity, emb_size):
    tokens, width = hidden.shape
    top_k = choice_t.shape[0]
    experts = w_router.shape[1]
    rows_hi = tokens * top_k // LANE
    dma = pltpu.SemaphoreType.DMA((emb_size - 1,))
    vmem = pl.BlockSpec(memory_space=pltpu.VMEM)
    return pl.pallas_call(
        functools.partial(prepare_kernel, capacity, emb_size, width * emb_size),
        out_shape=(
            jax.ShapeDtypeStruct((rows_hi, LANE), jnp.int32),
            jax.ShapeDtypeStruct((2, LANE), jnp.int32),
            jax.ShapeDtypeStruct((top_k, tokens), F32),
            jax.ShapeDtypeStruct((tokens, width), BF16),
            jax.ShapeDtypeStruct((experts, tokens), F32),
        ),
        in_specs=[vmem] * 4,
        out_specs=(vmem,) * 5,
        scratch_shapes=[pltpu.VMEM((emb_size, tokens // LANE, LANE), F32), dma, dma],
        compiler_params=pltpu.CompilerParams(collective_id=0, has_side_effects=True, vmem_limit_bytes=VMEM_BYTES),
        cost_estimate=cost(15e9, 4e6),
        name='prepare',
    )(choice_t, hidden, norm_pre.reshape(1, width), w_router)


def column_of(row):
    return jnp.transpose(jnp.broadcast_to(row, (LANE, LANE)))


def strips(tok, iota, count, axis):
    match = jnp.where(jnp.bitwise_and(tok, LANE - 1) == iota, 1.0, 0.0).astype(BF16)
    high = lax.shift_right_arithmetic(tok, 7).astype(F32).astype(BF16)
    zero = jnp.zeros_like(match)
    return jnp.concatenate([jnp.where(high == jnp.asarray(j, BF16), match, zero) for j in range(count)], axis=axis)


def grouped(seg_ref, step, in_ref, weights, out_ref):
    total = out_ref.shape[0]
    batch = len(weights)

    def block(e, w, offset):
        base = (seg_ref[0, e] // 16) * 16 + offset
        r0 = pl.multiple_of(jnp.minimum(base, total - ROW_BLOCK), 16)
        return r0, jnp.dot(in_ref[pl.ds(r0, ROW_BLOCK), :], w(), preferred_element_type=F32).astype(BF16)

    def put(r0, new, keep):
        row = r0 + lax.broadcasted_iota(jnp.int32, new.shape, 0)
        out_ref[pl.ds(r0, ROW_BLOCK), :] = jnp.where(keep(row), new, out_ref[pl.ds(r0, ROW_BLOCK), :])

    for q, (r0, new) in enumerate([block(step * batch + q, weights[q], 0) for q in range(batch)]):
        put(r0, new, lambda row: row >= seg_ref[0, step * batch + q])
    for q in range(batch):
        e = step * batch + q
        s, end = seg_ref[0, e], seg_ref[1, e]
        count = (end - (s // 16) * 16 + ROW_BLOCK - 1) // ROW_BLOCK

        def body(j, carry):
            r0, new = block(e, weights[q], j * ROW_BLOCK)
            put(r0, new, lambda row: jnp.logical_and(row >= s, row < end))
            return carry

        lax.fori_loop(1, count, body, 0)


def dispatch_up_kernel(steps, seg_ref, tok_ref, b_ref, wg_ref, wu_ref, z_ref, x_ref):
    i = pl.program_id(0)
    tokens = b_ref.shape[0]
    rows = x_ref.shape[0] // steps

    @pl.when(i < steps)
    def gather():
        lane = lax.broadcasted_iota(jnp.int32, (LANE, LANE), 1)
        pick = jnp.concatenate([
            strips(column_of(tok_ref[pl.ds(i * (rows // LANE) + q, 1), :]), lane, tokens // LANE, 1)
            for q in range(rows // LANE)], axis=0)
        at = pl.ds(pl.multiple_of(i * rows, rows), rows)
        x_ref[at, :] = jnp.dot(pick, b_ref[...], preferred_element_type=F32).astype(BF16)

    @pl.when(i >= steps)
    def project():
        pick = lambda q: lambda: jnp.concatenate([wg_ref[q], wu_ref[q]], axis=1)
        grouped(seg_ref, i - steps, x_ref, [pick(q) for q in range(wg_ref.shape[0])], z_ref)


def dispatch_up(seg, tok, b, w_gate, w_up):
    tokens, width = b.shape
    rows = tok.size
    experts, _, ffn = w_gate.shape
    steps = rows // 1024
    whole = lambda i, seg: (0, 0)
    one = pl.Buffered(1)
    w_spec = pl.BlockSpec((EXPERT_BATCH, width, ffn), lambda i, seg: (jnp.maximum(i - steps, 0), 0, 0))
    return pl.pallas_call(
        functools.partial(dispatch_up_kernel, steps),
        out_shape=jax.ShapeDtypeStruct((rows, 2 * ffn), BF16),
        grid_spec=pltpu.PrefetchScalarGridSpec(
            num_scalar_prefetch=1,
            grid=(steps + experts // EXPERT_BATCH,),
            in_specs=[pl.BlockSpec(tok.shape, whole, pipeline_mode=one), pl.BlockSpec(b.shape, whole, pipeline_mode=one), w_spec, w_spec],
            out_specs=pl.BlockSpec((rows, 2 * ffn), whole, pipeline_mode=one),
            scratch_shapes=[pltpu.VMEM((rows, width), BF16)],
        ),
        compiler_params=pltpu.CompilerParams(vmem_limit_bytes=VMEM_BYTES),
        cost_estimate=cost(2 * rows * width * (tokens + 2 * ffn), 8 * rows * width),
        name='dispatch_up',
    )(seg, tok, b, w_gate, w_up)


def exchange_kernel(emb_size, subs, z_ref, logit_ref, choice_ref, pos_ref, g_ref, gate_ref,
                    mine, theirs, ring, got, gates, load, send_p, recv_p, send_r, recv_r,
                    send_a, recv_a, send_d, recv_d, send_l, recv_l, send_g, recv_g):
    chips = emb_size // 2
    last = chips - 1
    me = lax.axis_index('emb')
    chip, core = me // 2, lax.rem(me, 2)
    partner = {'emb': chip * 2 + 1 - core}
    ways = [{'emb': lax.rem(me + 2, emb_size)}, {'emb': lax.rem(me + emb_size - 2, emb_size)}]
    own = z_ref.shape[0] // emb_size
    half = own // 2
    sub = half // subs
    ffn = g_ref.shape[1]
    greet({'emb': lax.rem(me + j, emb_size)} for j in range(1, emb_size))

    def around(c):
        return lax.rem(c + 2 * chips, chips)

    def target(d, step):
        return around(chip - 1 - step if d == 0 else chip + 1 + step)

    def rows(c, parity, d, u, size):
        return pl.ds(pl.multiple_of((c * 2 + parity) * own + d * half + u * sub, sub), size)

    order = [(step, u, d) for step in range(chips) for u in range(subs) for d in range(2)]
    loads, passed, sums = {}, {}, {}
    for step, u, d in order:
        c = target(d, step)
        copy = pltpu.make_async_remote_copy(
            src_ref=z_ref.at[rows(c, 1 - core, d, u, sub), :], dst_ref=theirs.at[step, d, u],
            send_sem=send_p.at[step, d, u], recv_sem=recv_p.at[step, d, u],
            device_id=partner, device_id_type=MESH)
        copy.start()
        passed[step, d, u] = copy
        copy = pltpu.make_async_copy(z_ref.at[rows(c, core, d, u, sub), :], mine.at[step, d, u], load.at[step, d, u])
        copy.start()
        loads[step, d, u] = copy

    experts, tokens = logit_ref.shape
    share_tok = tokens // emb_size

    def columns(who):
        return pl.ds(pl.multiple_of(who * share_tok, share_tok), share_tok)

    parts, picked = [], []
    for j in range(1, emb_size):
        peer = lax.rem(me + j, emb_size)
        parts.append(pltpu.make_async_remote_copy(
            src_ref=logit_ref.at[:, columns(peer)], dst_ref=got.at[j - 1],
            send_sem=send_l.at[j - 1], recv_sem=recv_l.at[j - 1],
            device_id={'emb': peer}, device_id_type=MESH))
        parts[-1].start()

    def pick_gates():
        logits = logit_ref[:, columns(me)]
        for j in range(1, emb_size):
            parts[j - 1].wait_recv()
            logits = logits + got[j - 1]
        grown = jnp.exp(logits - jnp.max(logits, axis=0, keepdims=True))
        prob = grown / jnp.sum(grown, axis=0, keepdims=True)
        e_iota = lax.broadcasted_iota(jnp.int32, (experts, share_tok), 0)
        chosen = choice_ref[:, columns(me)]
        for k in range(chosen.shape[0]):
            gate = jnp.sum(jnp.where(chosen[k:k + 1, :] == e_iota, prob, 0.0), axis=0, keepdims=True)
            gates[k:k + 1, columns(me)] = gate
        for j in range(1, emb_size):
            picked.append(pltpu.make_async_remote_copy(
                src_ref=gates.at[:, columns(me)], dst_ref=gates.at[:, columns(me)],
                send_sem=send_g.at[j - 1], recv_sem=recv_g.at[j - 1],
                device_id={'emb': lax.rem(me + j, emb_size)}, device_id_type=MESH))
            picked[-1].start()

    spread = {}

    def scatter(d, way, step, c, u):
        at = rows(c, core, d, u, sub)
        copy = pltpu.make_async_remote_copy(
            src_ref=g_ref.at[at, :], dst_ref=g_ref.at[at, :],
            send_sem=send_a.at[way, step, d, u], recv_sem=recv_a.at[way, step, d, u],
            device_id=ways[way], device_id_type=MESH)
        copy.start()
        spread[way, step, d, u] = copy

    across = {}

    def share(d, slot, c, u):
        at = rows(c, core, d, u, sub)
        copy = pltpu.make_async_remote_copy(
            src_ref=g_ref.at[at, :], dst_ref=g_ref.at[at, :],
            send_sem=send_d.at[slot, d, u], recv_sem=recv_d.at[slot, d, u],
            device_id=partner, device_id_type=MESH)
        copy.start()
        across[slot, d, u] = copy

    def sends(way, step, d):
        if step < (chips - 1) // 2:
            return True
        return step == (chips - 1) // 2 and chips % 2 == 0 and way == d

    piece = 32
    for step, u, d in order:
        if (u, d) == (0, 0) and step == 1:
            pick_gates()
        if (u, d) == (0, 0) and step == min(2, last):
            for copy in picked:
                copy.wait_recv()
            place_gates(pos_ref, gates, gate_ref)
        loads[step, d, u].wait()
        passed[step, d, u].wait_recv()
        if step >= 1:
            sums[step - 1, d, u].wait_recv()
        if step < last:
            def add(i, carry):
                at = pl.ds(pl.multiple_of(i * piece, piece), piece)
                v = mine[step, d, u, at, :].astype(F32) + theirs[step, d, u, at, :].astype(F32)
                if step >= 1:
                    v = v + ring[step - 1, d, u, at, :].astype(F32)
                mine[step, d, u, at, :] = v.astype(BF16)
                return carry

            lax.fori_loop(0, sub // piece, add, 0)
            copy = pltpu.make_async_remote_copy(
                src_ref=mine.at[step, d, u], dst_ref=ring.at[step, d, u],
                send_sem=send_r.at[step, d, u], recv_sem=recv_r.at[step, d, u],
                device_id=ways[d], device_id_type=MESH)
            copy.start()
            sums[step, d, u] = copy
        else:
            def act(i, carry):
                at = pl.ds(pl.multiple_of(i * piece, piece), piece)
                v = mine[step, d, u, at, :].astype(F32) + theirs[step, d, u, at, :].astype(F32)
                v = (v + ring[step - 1, d, u, at, :].astype(F32)).astype(BF16).astype(F32)
                v = jax.nn.gelu(v[:, :ffn], approximate=True) * v[:, ffn:]
                out = pl.ds(pl.multiple_of((chip * 2 + core) * own + d * half + u * sub + i * piece, piece), piece)
                g_ref[out, :] = v.astype(BF16)
                return carry

            lax.fori_loop(0, sub // piece, act, 0)
            for way in range(2):
                if sends(way, 0, d):
                    scatter(d, way, 0, chip, u)
            share(d, 0, chip, u)
    slot = 0
    for step in range(chips // 2):
        for u in range(subs):
            for way in range(2):
                for d in range(2):
                    if sends(way, step, d):
                        spread[way, step, d, u].wait_recv()
                        c = around(chip - 1 - step if way == 0 else chip + 1 + step)
                        if sends(way, step + 1, d):
                            scatter(d, way, step + 1, c, u)
                        full = sends(0, step, d) and sends(1, step, d)
                        share(d, 1 + 2 * step + (way if full else 0), c, u)
    for copy in across.values():
        copy.wait_recv()
    for group in (passed, sums, spread, across):
        for copy in group.values():
            copy.wait_send()
    for copy in parts + picked:
        copy.wait_send()


def exchange(z, logits, choice_t, pos, emb_size):
    rows, both = z.shape
    experts, tokens = logits.shape
    vmem = pl.BlockSpec(memory_space=pltpu.VMEM)
    peers = pltpu.SemaphoreType.DMA((emb_size - 1,))
    chips = emb_size // 2
    own = rows // emb_size
    subs = 4
    sub = own // (2 * subs)
    dma = pltpu.SemaphoreType.DMA
    part = (chips, 2, subs)
    hop = (chips - 1, 2, subs)
    fan = (2, max(chips // 2, 1), 2, subs)
    return pl.pallas_call(
        functools.partial(exchange_kernel, emb_size, subs),
        out_shape=(jax.ShapeDtypeStruct((rows, both // 2), BF16), jax.ShapeDtypeStruct((rows // LANE, LANE), F32)),
        in_specs=[pl.BlockSpec(memory_space=pl.ANY), vmem, vmem, vmem],
        out_specs=(vmem, vmem),
        scratch_shapes=[
            pltpu.VMEM(part + (sub, both), BF16),
            pltpu.VMEM(part + (sub, both), BF16),
            pltpu.VMEM(hop + (sub, both), BF16),
            pltpu.VMEM((emb_size - 1, experts, tokens // emb_size), F32),
            pltpu.VMEM(choice_t.shape, F32),
            dma(part), dma(part), dma(part), dma(hop), dma(hop), dma(fan), dma(fan), dma(part), dma(part),
            peers, peers, peers, peers,
        ],
        compiler_params=pltpu.CompilerParams(collective_id=2, has_side_effects=True, vmem_limit_bytes=VMEM_BYTES),
        cost_estimate=cost(100e9, 4 * rows * both),
        name='exchange',
    )(z, logits, choice_t, pos)


def place_gates(pos_ref, gates, gate_ref):
    top_k = pos_ref.shape[0]
    rows_hi = gate_ref.shape[0]
    acc = jnp.zeros((rows_hi, 3 * LANE), F32)
    for k in range(top_k):
        is_hi, is_lo = onehot_pieces(pos_ref[k:k + 1, :], rows_hi)
        left = jnp.where(is_hi, 1.0, 0.0).astype(BF16)
        pieces = []
        rest = gates[k:k + 1, :]
        for _ in range(3):
            piece = rest.astype(BF16).astype(F32)
            rest = rest - piece
            pieces.append(jnp.where(is_lo, piece, 0.0).astype(BF16))
        right = jnp.concatenate(pieces, axis=0)
        acc += lax.dot_general(left, right, (((1,), (1,)), ((), ())), preferred_element_type=F32)
    gate_ref[...] = acc[:, :LANE] + acc[:, LANE:2 * LANE] + acc[:, 2 * LANE:]


def finish_kernel(ffn_size, emb_size, model_width, u_ref, tok_ref, hid_ref, post_ref, out_ref, rows_u, part, got,
                  total, squares, load, send_a, recv_a, send_b, recv_b, send_c, recv_c):
    tokens, width = out_ref.shape
    own = tokens // ffn_size
    half = own // 2
    subs = got.shape[2]
    sub = half // subs
    last = ffn_size - 1
    me = lax.axis_index('ffn')
    emb = lax.axis_index('emb')
    peers = [{'ffn': lax.rem(me + 1, ffn_size)}, {'ffn': lax.rem(me + ffn_size - 1, ffn_size)}]
    blocks = load.shape[0]
    size = rows_u.shape[0] // blocks

    def fetch(i):
        at = pl.ds(pl.multiple_of(i * size, size), size)
        return pltpu.make_async_copy(u_ref.at[at, :], rows_u.at[at, :], load.at[i])

    for i in range(blocks):
        fetch(i).start()
    greet(peers + [{'emb': lax.rem(emb + j, emb_size)} for j in range(1, emb_size)])
    t_iota = lax.broadcasted_iota(jnp.int32, (half, LANE), 0)

    def combine(d, step):
        chunk = me - 1 - step if d == 0 else me + 1 + step
        first = lax.rem(chunk + ffn_size * 2, ffn_size) * own + d * half
        part[d, step] = jnp.zeros((half, width), F32)

        def body(i, carry):
            if (d, step) == (0, 0):
                fetch(i).wait()
            pick = jnp.concatenate([
                jnp.where(tok_ref[pl.ds(i * (size // LANE) + q, 1), :] - first == t_iota, 1.0, 0.0).astype(BF16)
                for q in range(size // LANE)], axis=1)
            at = pl.ds(pl.multiple_of(i * size, size), size)
            part[d, step] = part[d, step] + jnp.dot(pick, rows_u[at, :], preferred_element_type=F32)
            return carry

        lax.fori_loop(0, blocks, body, 0)

    sums = {}
    for step in range(ffn_size):
        for d in range(2):
            combine(d, step)
        for u in range(subs):
            for d in range(2):
                at = pl.ds(u * sub, sub)
                if step >= 1:
                    sums[d, step - 1, u].wait_recv()
                    value = got[d, step - 1, u] + part[d, step, at, :]
                    if step == last:
                        total[d * half + u * sub:d * half + (u + 1) * sub, :] = value
                    else:
                        got[d, step - 1, u] = value
                if step < last:
                    copy = pltpu.make_async_remote_copy(
                        src_ref=part.at[d, 0, at, :] if step == 0 else got.at[d, step - 1, u], dst_ref=got.at[d, step, u],
                        send_sem=send_a.at[d, step, u], recv_sem=recv_a.at[d, step, u],
                        device_id=peers[d], device_id_type=MESH)
                    copy.start()
                    sums[d, step, u] = copy
    for i in range(own // LANE):
        squares[emb_size - 1, i:i + 1, :] = square_rows(total[i * LANE:(i + 1) * LANE, :])
    shares = share_squares(squares, emb_size, send_b, recv_b)
    for copy in shares:
        copy.wait_recv()
    inv = inverse_rms(squares, emb_size, model_width)
    post = post_ref[...].astype(F32)

    def rows(chunk, start, size):
        chunk = lax.rem(chunk + ffn_size * 2, ffn_size)
        return pl.ds(pl.multiple_of(chunk * own + start, size), size)

    for i in range(own // LANE):
        col = jnp.concatenate([column_of(inv[i:i + 1, :])] * (width // LANE), axis=1)
        at = rows(me, i * LANE, LANE)
        out_ref[at, :] = (hid_ref[at, :].astype(F32) + total[i * LANE:(i + 1) * LANE, :] * col * post).astype(BF16)
    spread = []
    for step in range(ffn_size // 2):
        if step >= 1:
            for copy in spread[-2:]:
                copy.wait_recv()
        last = step == (ffn_size - 1) // 2
        for d in range(2):
            chunk = me - step if d == 0 else me + step
            at = rows(chunk, d * own // 2, own // 2) if last else rows(chunk, 0, own)
            spread.append(pltpu.make_async_remote_copy(
                src_ref=out_ref.at[at, :], dst_ref=out_ref.at[at, :],
                send_sem=send_c.at[d, step], recv_sem=recv_c.at[d, step],
                device_id=peers[d], device_id_type=MESH))
            spread[-1].start()
    for copy in spread[-2:]:
        copy.wait_recv()
    for copy in list(sums.values()) + shares + spread:
        copy.wait_send()


def finish(u, tok, hidden, norm_post, ffn_size, emb_size):
    tokens, width = hidden.shape
    rows = u.shape[0]
    own = tokens // ffn_size
    half = own // 2
    subs = 2 if half % 256 == 0 else 1
    vmem = pl.BlockSpec(memory_space=pltpu.VMEM)
    dma = pltpu.SemaphoreType.DMA
    hops = (2, ffn_size - 1, subs)
    return pl.pallas_call(
        functools.partial(finish_kernel, ffn_size, emb_size, width * emb_size),
        out_shape=jax.ShapeDtypeStruct((tokens, width), BF16),
        in_specs=[pl.BlockSpec(memory_space=pl.ANY), vmem, vmem, vmem],
        out_specs=vmem,
        scratch_shapes=[
            pltpu.VMEM((rows, width), BF16),
            pltpu.VMEM((2, ffn_size, half, width), F32),
            pltpu.VMEM(hops + (half // subs, width), F32),
            pltpu.VMEM((own, width), F32),
            pltpu.VMEM((emb_size, own // LANE, LANE), F32),
            dma((rows // 2048,)), dma(hops), dma(hops),
            dma((emb_size - 1,)), dma((emb_size - 1,)),
            dma((2, ffn_size // 2)), dma((2, ffn_size // 2)),
        ],
        compiler_params=pltpu.CompilerParams(collective_id=1, has_side_effects=True, vmem_limit_bytes=VMEM_BYTES),
        cost_estimate=cost(2 * rows * tokens * width, 16e6),
        name='finish',
    )(u, tok, hidden, norm_post.reshape(1, width))


def down_kernel(seg_ref, gate_ref, g_ref, w_ref, u_ref):
    width = u_ref.shape[1]
    pick = lambda q: lambda: w_ref[q]
    grouped(seg_ref, pl.program_id(0), g_ref, [pick(q) for q in range(w_ref.shape[0])], u_ref)

    @pl.when(pl.program_id(0) == pl.num_programs(0) - 1)
    def scale():
        def body(i, carry):
            for q in range(4):
                hi = i * 4 + q
                col = jnp.concatenate([column_of(gate_ref[pl.ds(hi, 1), :])] * (width // LANE), axis=1)
                at = pl.ds(pl.multiple_of(hi * LANE, LANE), LANE)
                u_ref[at, :] = (u_ref[at, :].astype(F32) * col).astype(BF16)
            return carry

        lax.fori_loop(0, gate_ref.shape[0] // 4, body, 0)


def expert_down(seg, gate, act, w_down):
    rows, ffn = act.shape
    experts, _, width = w_down.shape
    whole = lambda e, seg: (0, 0)
    one = pl.Buffered(1)
    return pl.pallas_call(
        down_kernel,
        out_shape=jax.ShapeDtypeStruct((rows, width), BF16),
        grid_spec=pltpu.PrefetchScalarGridSpec(
            num_scalar_prefetch=1,
            grid=(experts // EXPERT_BATCH,),
            in_specs=[
                pl.BlockSpec(gate.shape, whole, pipeline_mode=one),
                pl.BlockSpec(act.shape, whole, pipeline_mode=one),
                pl.BlockSpec((EXPERT_BATCH, ffn, width), lambda e, seg: (e, 0, 0)),
            ],
            out_specs=pl.BlockSpec((rows, width), whole, pipeline_mode=one),
        ),
        compiler_params=pltpu.CompilerParams(vmem_limit_bytes=VMEM_BYTES),
        cost_estimate=cost(2 * rows * width * ffn, 4 * rows * width),
        name='expert_down',
    )(seg, gate, act, w_down)


def solution(mesh):
    emb_size = mesh.shape['emb']
    ffn_size = mesh.shape['ffn']

    def local_block(hidden, norm_pre, norm_post, w_router, w_gate, w_up, w_down, choice):
        num_tok, local_width = hidden.shape
        experts = w_gate.shape[0]
        top_k = choice.shape[1]
        capacity = 2 * num_tok * top_k // experts
        choice_t = choice.T
        tok, seg, pos, normed, logits = prepare(choice_t, hidden, norm_pre, w_router, capacity, emb_size)
        z = dispatch_up(seg, tok, normed, w_gate, w_up)
        act, gate = exchange(z, logits, choice_t, pos, emb_size)
        u = expert_down(seg, gate, act, w_down)
        return finish(u, tok, hidden, norm_post, ffn_size, emb_size)

    in_specs = (P('dp', 'emb'), P('emb'), P('emb'), P('emb', None), P(None, 'emb', 'ffn'), P(None, 'emb', 'ffn'), P(None, 'ffn', 'emb'), P('dp', None))
    return jax.shard_map(local_block, mesh=mesh, in_specs=in_specs, out_specs=P('dp', 'emb'), check_vma=False)
```

```python
import functools

import jax
import jax.numpy as jnp
from jax import lax
from jax.experimental import pallas as pl
from jax.experimental.pallas import tpu as pltpu
from jax.sharding import PartitionSpec as P

EPS = 1e-5
LANE = 128
ROW_BLOCK = 272
EXPERT_BATCH = 8
VMEM_BYTES = 60 * 1024 * 1024
F32 = jnp.float32
BF16 = jnp.bfloat16
MESH = pl.DeviceIdType.MESH


def cost(flops, nbytes):
    return pl.CostEstimate(flops=int(flops), bytes_accessed=int(nbytes), transcendentals=0)


def greet(peers):
    barrier = pltpu.get_barrier_semaphore()
    count = 0
    for peer in peers:
        pl.semaphore_signal(barrier, inc=1, device_id=peer, device_id_type=MESH)
        count += 1
    pl.semaphore_wait(barrier, count)


def onehot_pieces(pos_row, rows_hi):
    tokens = pos_row.shape[1]
    hi = jnp.floor(pos_row * (1.0 / LANE))
    lo = pos_row - hi * LANE
    hi_iota = lax.broadcasted_iota(jnp.int32, (rows_hi, tokens), 0).astype(F32)
    lo_iota = lax.broadcasted_iota(jnp.int32, (LANE, tokens), 0).astype(F32)
    return hi == hi_iota, lo == lo_iota


def route_rows(capacity, experts, choice_ref, tok_ref, seg_ref, pos_ref):
    top_k, tokens = choice_ref.shape
    rows_hi = tok_ref.shape[0]
    rows = rows_hi * LANE
    blk = 256
    e_iota = lax.broadcasted_iota(jnp.int32, (experts, tokens), 0)
    assigned = jnp.zeros((experts, tokens), F32)
    for k in range(top_k):
        assigned += jnp.where(choice_ref[k:k + 1, :] == e_iota, 1.0, 0.0)
    r_i = lax.broadcasted_iota(jnp.int32, (blk, blk), 0)
    c_i = lax.broadcasted_iota(jnp.int32, (blk, blk), 1)
    tri = jnp.where(r_i < c_i, 1.0, 0.0).astype(BF16)
    carry = jnp.zeros((experts, 1), F32)
    before = []
    for b in range(tokens // blk):
        part = assigned[:, b * blk:(b + 1) * blk]
        within = jnp.dot(part.astype(BF16), tri, preferred_element_type=F32)
        before.append(within + carry)
        carry = carry + jnp.sum(part, axis=1, keepdims=True)
    before = jnp.concatenate(before, axis=1)
    kept = jnp.broadcast_to(jnp.minimum(carry, float(capacity)), (experts, LANE))
    kept_hi = jnp.floor(kept * (1.0 / 16.0))
    kept_lo = kept - kept_hi * 16.0
    er = lax.broadcasted_iota(jnp.int32, (experts, experts), 0)
    ec = lax.broadcasted_iota(jnp.int32, (experts, experts), 1)
    low = jnp.where(ec < er, 1.0, 0.0).astype(BF16)
    start = 16.0 * jnp.dot(low, kept_hi.astype(BF16), preferred_element_type=F32)
    start = start + jnp.dot(low, kept_lo.astype(BF16), preferred_element_type=F32)
    end = start + kept
    fill = jnp.zeros((LANE - experts, LANE), F32)
    start_t = jnp.transpose(jnp.concatenate([start, fill], axis=0))
    end_t = jnp.transpose(jnp.concatenate([end, fill], axis=0))
    seg_ref[0:1, :] = start_t[0:1, :].astype(jnp.int32)
    lane = lax.broadcasted_iota(jnp.int32, (1, LANE), 1)
    seg_ref[1:2, :] = jnp.where(lane == experts - 1, rows, end_t[0:1, :].astype(jnp.int32))
    value = jnp.where(before < capacity, before + start[:, 0:1], float(rows))
    t_val = lax.broadcasted_iota(jnp.int32, (1, tokens), 1) + 1
    t_hi = (t_val // 16).astype(F32)
    t_lo = (t_val % 16).astype(F32)
    acc = jnp.zeros((rows_hi, 2 * LANE), F32)
    for k in range(top_k):
        hit = choice_ref[k:k + 1, :] == e_iota
        pos = jnp.sum(jnp.where(hit, value, 0.0), axis=0, keepdims=True)
        pos_ref[k:k + 1, :] = pos
        is_hi, is_lo = onehot_pieces(pos, rows_hi)
        left = jnp.where(is_hi, 1.0, 0.0).astype(BF16)
        right = jnp.concatenate([jnp.where(is_lo, t_hi, 0.0), jnp.where(is_lo, t_lo, 0.0)], axis=0).astype(BF16)
        acc += lax.dot_general(left, right, (((1,), (1,)), ((), ())), preferred_element_type=F32)
    tok_ref[...] = (16.0 * acc[:, :LANE] + acc[:, LANE:]).astype(jnp.int32) - 1


def square_rows(block):
    block = block * block
    lanes = block[:, :LANE]
    for j in range(1, block.shape[1] // LANE):
        lanes = lanes + block[:, j * LANE:(j + 1) * LANE]
    return jnp.sum(jnp.transpose(lanes), axis=0, keepdims=True)


def share_squares(squares, emb_size, send, recv):
    me = lax.axis_index('emb')
    copies = []
    for j in range(1, emb_size):
        copies.append(pltpu.make_async_remote_copy(
            src_ref=squares.at[emb_size - 1], dst_ref=squares.at[j - 1],
            send_sem=send.at[j - 1], recv_sem=recv.at[j - 1],
            device_id={'emb': lax.rem(me + j, emb_size)}, device_id_type=MESH))
        copies[-1].start()
    return copies


def inverse_rms(squares, emb_size, model_width):
    whole = squares[emb_size - 1]
    for j in range(emb_size - 1):
        whole = whole + squares[j]
    return lax.rsqrt(whole / model_width + EPS)


def prepare_kernel(capacity, emb_size, model_width, choice_ref, hid_ref, pre_ref, wr_ref,
                   tok_ref, seg_ref, pos_ref, b_ref, logit_ref, squares, send, recv):
    tokens, width = hid_ref.shape
    me = lax.axis_index('emb')
    greet({'emb': lax.rem(me + j, emb_size)} for j in range(1, emb_size))
    for i in range(tokens // LANE):
        squares[emb_size - 1, i:i + 1, :] = square_rows(hid_ref[i * LANE:(i + 1) * LANE, :].astype(F32))
    copies = share_squares(squares, emb_size, send, recv)
    route_rows(capacity, wr_ref.shape[0], choice_ref, tok_ref, seg_ref, pos_ref)
    for copy in copies:
        copy.wait_recv()
    inv = inverse_rms(squares, emb_size, model_width)
    pre = pre_ref[...].reshape(1, width).astype(F32)
    for i in range(tokens // LANE):
        col = jnp.concatenate([column_of(inv[i:i + 1, :])] * (width // LANE), axis=1)
        part = slice(i * LANE, (i + 1) * LANE)
        b_ref[part, :] = (hid_ref[part, :].astype(F32) * col * pre).astype(BF16)
    logit_ref[...] = lax.dot_general(wr_ref[...], b_ref[...], (((1,), (1,)), ((), ())), preferred_element_type=F32)
    for copy in copies:
        copy.wait_send()


def prepare(choice_t, hidden, norm_pre, w_router, capacity, emb_size):
    tokens, width = hidden.shape
    top_k = choice_t.shape[0]
    experts = w_router.shape[1]
    rows_hi = tokens * top_k // LANE
    dma = pltpu.SemaphoreType.DMA((emb_size - 1,))
    vmem = pl.BlockSpec(memory_space=pltpu.VMEM)
    return pl.pallas_call(
        functools.partial(prepare_kernel, capacity, emb_size, width * emb_size),
        out_shape=(
            jax.ShapeDtypeStruct((rows_hi, LANE), jnp.int32),
            jax.ShapeDtypeStruct((2, LANE), jnp.int32),
            jax.ShapeDtypeStruct((top_k, tokens), F32),
            jax.ShapeDtypeStruct((tokens, width), BF16),
            jax.ShapeDtypeStruct((experts, tokens), F32),
        ),
        in_specs=[vmem] * 4,
        out_specs=(vmem,) * 5,
        scratch_shapes=[pltpu.VMEM((emb_size, tokens // LANE, LANE), F32), dma, dma],
        compiler_params=pltpu.CompilerParams(collective_id=0, has_side_effects=True, vmem_limit_bytes=VMEM_BYTES),
        cost_estimate=cost(15e9, 4e6),
        name='prepare',
    )(choice_t, hidden, norm_pre, w_router.T)


def column_of(row):
    return jnp.transpose(jnp.broadcast_to(row, (LANE, LANE)))


def strips(tok, iota, count, axis):
    match = jnp.where(jnp.bitwise_and(tok, LANE - 1) == iota, 1.0, 0.0).astype(BF16)
    high = lax.shift_right_arithmetic(tok, 7).astype(F32).astype(BF16)
    zero = jnp.zeros_like(match)
    return jnp.concatenate([jnp.where(high == jnp.asarray(j, BF16), match, zero) for j in range(count)], axis=axis)


def grouped(seg_ref, step, in_ref, weights, out_ref):
    batch = len(weights)

    def block(e, w, offset):
        r0 = pl.multiple_of((seg_ref[0, e] // 16) * 16 + offset, 16)
        return r0, jnp.dot(in_ref[pl.ds(r0, ROW_BLOCK), :], w(), preferred_element_type=F32).astype(BF16)

    for q in range(batch):
        e = step * batch + q
        r0, new = block(e, weights[q], 0)
        head = out_ref[pl.ds(r0, 16), :]
        row = r0 + lax.broadcasted_iota(jnp.int32, head.shape, 0)
        out_ref[pl.ds(r0, 16), :] = jnp.where(row >= seg_ref[0, e], new[:16, :], head)
        out_ref[pl.ds(r0 + 16, ROW_BLOCK - 16), :] = new[16:, :]
    for q in range(batch):
        e = step * batch + q
        s, end = seg_ref[0, e], seg_ref[1, e]
        count = (end - (s // 16) * 16 + ROW_BLOCK - 1) // ROW_BLOCK

        def body(j, carry):
            r0, new = block(e, weights[q], j * ROW_BLOCK)
            row = r0 + lax.broadcasted_iota(jnp.int32, new.shape, 0)
            keep = jnp.logical_and(row >= s, row < end)
            out_ref[pl.ds(r0, ROW_BLOCK), :] = jnp.where(keep, new, out_ref[pl.ds(r0, ROW_BLOCK), :])
            return carry

        lax.fori_loop(1, count, body, 0)


def dispatch_up_kernel(steps, seg_ref, tok_ref, b_ref, wg_ref, wu_ref, z_ref, x_ref):
    i = pl.program_id(0)
    tokens = b_ref.shape[0]
    rows = (x_ref.shape[0] - ROW_BLOCK) // steps

    @pl.when(i < steps)
    def gather():
        lane = lax.broadcasted_iota(jnp.int32, (LANE, LANE), 1)
        pick = jnp.concatenate([
            strips(column_of(tok_ref[pl.ds(i * (rows // LANE) + q, 1), :]), lane, tokens // LANE, 1)
            for q in range(rows // LANE)], axis=0)
        at = pl.ds(pl.multiple_of(i * rows, rows), rows)
        x_ref[at, :] = jnp.dot(pick, b_ref[...], preferred_element_type=F32).astype(BF16)

    @pl.when(i >= steps)
    def project():
        pick = lambda q: lambda: jnp.concatenate([wg_ref[q], wu_ref[q]], axis=1)
        grouped(seg_ref, i - steps, x_ref, [pick(q) for q in range(wg_ref.shape[0])], z_ref)


def dispatch_up(seg, tok, b, w_gate, w_up):
    tokens, width = b.shape
    rows = tok.size
    experts, _, ffn = w_gate.shape
    steps = rows // 1024
    whole = lambda i, seg: (0, 0)
    one = pl.Buffered(1)
    w_spec = pl.BlockSpec((EXPERT_BATCH, width, ffn), lambda i, seg: (jnp.maximum(i - steps, 0), 0, 0))
    return pl.pallas_call(
        functools.partial(dispatch_up_kernel, steps),
        out_shape=jax.ShapeDtypeStruct((rows + ROW_BLOCK, 2 * ffn), BF16),
        grid_spec=pltpu.PrefetchScalarGridSpec(
            num_scalar_prefetch=1,
            grid=(steps + experts // EXPERT_BATCH,),
            in_specs=[pl.BlockSpec(tok.shape, whole, pipeline_mode=one), pl.BlockSpec(b.shape, whole, pipeline_mode=one), w_spec, w_spec],
            out_specs=pl.BlockSpec((rows + ROW_BLOCK, 2 * ffn), whole, pipeline_mode=one),
            scratch_shapes=[pltpu.VMEM((rows + ROW_BLOCK, width), BF16)],
        ),
        compiler_params=pltpu.CompilerParams(vmem_limit_bytes=VMEM_BYTES),
        cost_estimate=cost(2 * rows * width * (tokens + 2 * ffn), 8 * rows * width),
        name='dispatch_up',
    )(seg, tok, b, w_gate, w_up)


def exchange_kernel(emb_size, subs, z_ref, logit_ref, choice_ref, pos_ref, g_ref, gate_ref,
                    mine, theirs, ring, got, gates, load, send_p, recv_p, send_r, recv_r,
                    send_a, recv_a, send_d, recv_d, send_l, recv_l, send_g, recv_g):
    chips = emb_size // 2
    last = chips - 1
    me = lax.axis_index('emb')
    chip, core = me // 2, lax.rem(me, 2)
    partner = {'emb': chip * 2 + 1 - core}
    ways = [{'emb': lax.rem(me + 2, emb_size)}, {'emb': lax.rem(me + emb_size - 2, emb_size)}]
    own = gate_ref.size // emb_size
    half = own // 2
    sub = half // subs
    ffn = g_ref.shape[1]
    greet({'emb': lax.rem(me + j, emb_size)} for j in range(1, emb_size))

    def around(c):
        return lax.rem(c + 2 * chips, chips)

    def target(d, step):
        return around(chip - 1 - step if d == 0 else chip + 1 + step)

    def rows(c, parity, d, u, size):
        return pl.ds(pl.multiple_of((c * 2 + parity) * own + d * half + u * sub, sub), size)

    order = [(step, u, d) for step in range(chips) for u in range(subs) for d in range(2)]
    loads, passed, sums = {}, {}, {}
    for step, u, d in order:
        c = target(d, step)
        copy = pltpu.make_async_remote_copy(
            src_ref=z_ref.at[rows(c, 1 - core, d, u, sub), :], dst_ref=theirs.at[step, d, u],
            send_sem=send_p.at[step, d, u], recv_sem=recv_p.at[step, d, u],
            device_id=partner, device_id_type=MESH)
        copy.start()
        passed[step, d, u] = copy
        copy = pltpu.make_async_copy(z_ref.at[rows(c, core, d, u, sub), :], mine.at[step, d, u], load.at[step, d, u])
        copy.start()
        loads[step, d, u] = copy

    experts, tokens = logit_ref.shape
    share_tok = tokens // emb_size

    def columns(who):
        return pl.ds(pl.multiple_of(who * share_tok, share_tok), share_tok)

    parts, picked = [], []
    for j in range(1, emb_size):
        peer = lax.rem(me + j, emb_size)
        parts.append(pltpu.make_async_remote_copy(
            src_ref=logit_ref.at[:, columns(peer)], dst_ref=got.at[j - 1],
            send_sem=send_l.at[j - 1], recv_sem=recv_l.at[j - 1],
            device_id={'emb': peer}, device_id_type=MESH))
        parts[-1].start()

    def pick_gates():
        logits = logit_ref[:, columns(me)]
        for j in range(1, emb_size):
            parts[j - 1].wait_recv()
            logits = logits + got[j - 1]
        grown = jnp.exp(logits - jnp.max(logits, axis=0, keepdims=True))
        prob = grown / jnp.sum(grown, axis=0, keepdims=True)
        e_iota = lax.broadcasted_iota(jnp.int32, (experts, share_tok), 0)
        chosen = choice_ref[:, columns(me)]
        for k in range(chosen.shape[0]):
            gate = jnp.sum(jnp.where(chosen[k:k + 1, :] == e_iota, prob, 0.0), axis=0, keepdims=True)
            gates[k:k + 1, columns(me)] = gate
        for j in range(1, emb_size):
            picked.append(pltpu.make_async_remote_copy(
                src_ref=gates.at[:, columns(me)], dst_ref=gates.at[:, columns(me)],
                send_sem=send_g.at[j - 1], recv_sem=recv_g.at[j - 1],
                device_id={'emb': lax.rem(me + j, emb_size)}, device_id_type=MESH))
            picked[-1].start()

    spread = {}

    def scatter(d, way, step, c, u):
        at = rows(c, core, d, u, sub)
        copy = pltpu.make_async_remote_copy(
            src_ref=g_ref.at[at, :], dst_ref=g_ref.at[at, :],
            send_sem=send_a.at[way, step, d, u], recv_sem=recv_a.at[way, step, d, u],
            device_id=ways[way], device_id_type=MESH)
        copy.start()
        spread[way, step, d, u] = copy

    across = {}

    def share(d, slot, c, u):
        at = rows(c, core, d, u, sub)
        copy = pltpu.make_async_remote_copy(
            src_ref=g_ref.at[at, :], dst_ref=g_ref.at[at, :],
            send_sem=send_d.at[slot, d, u], recv_sem=recv_d.at[slot, d, u],
            device_id=partner, device_id_type=MESH)
        copy.start()
        across[slot, d, u] = copy

    def sends(way, step, d):
        if step < (chips - 1) // 2:
            return True
        return step == (chips - 1) // 2 and chips % 2 == 0 and way == d

    piece = 32
    for step, u, d in order:
        if (u, d) == (0, 0) and step == 1:
            pick_gates()
        if (u, d) == (0, 0) and step == min(2, last):
            for copy in picked:
                copy.wait_recv()
            place_gates(pos_ref, gates, gate_ref)
        loads[step, d, u].wait()
        passed[step, d, u].wait_recv()
        if step >= 1:
            sums[step - 1, d, u].wait_recv()
        if step < last:
            def add(i, carry):
                at = pl.ds(pl.multiple_of(i * piece, piece), piece)
                v = mine[step, d, u, at, :].astype(F32) + theirs[step, d, u, at, :].astype(F32)
                if step >= 1:
                    v = v + ring[step - 1, d, u, at, :].astype(F32)
                mine[step, d, u, at, :] = v.astype(BF16)
                return carry

            lax.fori_loop(0, sub // piece, add, 0)
            copy = pltpu.make_async_remote_copy(
                src_ref=mine.at[step, d, u], dst_ref=ring.at[step, d, u],
                send_sem=send_r.at[step, d, u], recv_sem=recv_r.at[step, d, u],
                device_id=ways[d], device_id_type=MESH)
            copy.start()
            sums[step, d, u] = copy
        else:
            def act(i, carry):
                at = pl.ds(pl.multiple_of(i * piece, piece), piece)
                v = mine[step, d, u, at, :].astype(F32) + theirs[step, d, u, at, :].astype(F32)
                v = (v + ring[step - 1, d, u, at, :].astype(F32)).astype(BF16).astype(F32)
                v = jax.nn.gelu(v[:, :ffn], approximate=True) * v[:, ffn:]
                out = pl.ds(pl.multiple_of((chip * 2 + core) * own + d * half + u * sub + i * piece, piece), piece)
                g_ref[out, :] = v.astype(BF16)
                return carry

            lax.fori_loop(0, sub // piece, act, 0)
            for way in range(2):
                if sends(way, 0, d):
                    scatter(d, way, 0, chip, u)
            share(d, 0, chip, u)
    slot = 0
    for step in range(chips // 2):
        for u in range(subs):
            for way in range(2):
                for d in range(2):
                    if sends(way, step, d):
                        spread[way, step, d, u].wait_recv()
                        c = around(chip - 1 - step if way == 0 else chip + 1 + step)
                        if sends(way, step + 1, d):
                            scatter(d, way, step + 1, c, u)
                        full = sends(0, step, d) and sends(1, step, d)
                        share(d, 1 + 2 * step + (way if full else 0), c, u)
    for copy in across.values():
        copy.wait_recv()
    for group in (passed, sums, spread, across):
        for copy in group.values():
            copy.wait_send()
    for copy in parts + picked:
        copy.wait_send()


def exchange(z, logits, choice_t, pos, emb_size):
    rows, both = choice_t.size, z.shape[1]
    experts, tokens = logits.shape
    vmem = pl.BlockSpec(memory_space=pltpu.VMEM)
    peers = pltpu.SemaphoreType.DMA((emb_size - 1,))
    chips = emb_size // 2
    own = rows // emb_size
    subs = 4
    sub = own // (2 * subs)
    dma = pltpu.SemaphoreType.DMA
    part = (chips, 2, subs)
    hop = (chips - 1, 2, subs)
    fan = (2, max(chips // 2, 1), 2, subs)
    return pl.pallas_call(
        functools.partial(exchange_kernel, emb_size, subs),
        out_shape=(jax.ShapeDtypeStruct((rows + ROW_BLOCK, both // 2), BF16), jax.ShapeDtypeStruct((rows // LANE, LANE), F32)),
        in_specs=[pl.BlockSpec(memory_space=pl.ANY), vmem, vmem, vmem],
        out_specs=(vmem, vmem),
        scratch_shapes=[
            pltpu.VMEM(part + (sub, both), BF16),
            pltpu.VMEM(part + (sub, both), BF16),
            pltpu.VMEM(hop + (sub, both), BF16),
            pltpu.VMEM((emb_size - 1, experts, tokens // emb_size), F32),
            pltpu.VMEM(choice_t.shape, F32),
            dma(part), dma(part), dma(part), dma(hop), dma(hop), dma(fan), dma(fan), dma(part), dma(part),
            peers, peers, peers, peers,
        ],
        compiler_params=pltpu.CompilerParams(collective_id=2, has_side_effects=True, vmem_limit_bytes=VMEM_BYTES),
        cost_estimate=cost(100e9, 4 * rows * both),
        name='exchange',
    )(z, logits, choice_t, pos)


def place_gates(pos_ref, gates, gate_ref):
    top_k = pos_ref.shape[0]
    rows_hi = gate_ref.shape[0]
    acc = jnp.zeros((rows_hi, 3 * LANE), F32)
    for k in range(top_k):
        is_hi, is_lo = onehot_pieces(pos_ref[k:k + 1, :], rows_hi)
        left = jnp.where(is_hi, 1.0, 0.0).astype(BF16)
        pieces = []
        rest = gates[k:k + 1, :]
        for _ in range(3):
            piece = rest.astype(BF16).astype(F32)
            rest = rest - piece
            pieces.append(jnp.where(is_lo, piece, 0.0).astype(BF16))
        right = jnp.concatenate(pieces, axis=0)
        acc += lax.dot_general(left, right, (((1,), (1,)), ((), ())), preferred_element_type=F32)
    gate_ref[...] = acc[:, :LANE] + acc[:, LANE:2 * LANE] + acc[:, 2 * LANE:]


def finish_kernel(ffn_size, emb_size, model_width, u_ref, tok_ref, hid_ref, post_ref, out_ref, rows_u, part, got,
                  total, squares, load, send_a, recv_a, send_b, recv_b, send_c, recv_c):
    tokens, width = out_ref.shape
    own = tokens // ffn_size
    half = own // 2
    subs = got.shape[2]
    sub = half // subs
    last = ffn_size - 1
    me = lax.axis_index('ffn')
    emb = lax.axis_index('emb')
    peers = [{'ffn': lax.rem(me + 1, ffn_size)}, {'ffn': lax.rem(me + ffn_size - 1, ffn_size)}]
    blocks = load.shape[0]
    size = rows_u.shape[0] // blocks

    def fetch(i):
        at = pl.ds(pl.multiple_of(i * size, size), size)
        return pltpu.make_async_copy(u_ref.at[at, :], rows_u.at[at, :], load.at[i])

    for i in range(blocks):
        fetch(i).start()
    greet(peers + [{'emb': lax.rem(emb + j, emb_size)} for j in range(1, emb_size)])
    t_iota = lax.broadcasted_iota(jnp.int32, (half, LANE), 0)

    def combine(step):
        firsts = []
        for d in range(2):
            chunk = me - 1 - step if d == 0 else me + 1 + step
            firsts.append(lax.rem(chunk + ffn_size * 2, ffn_size) * own + d * half)
            part[d, step] = jnp.zeros((half, width), F32)

        def body(i, carry):
            if step == 0:
                fetch(i).wait()
            tok = [tok_ref[pl.ds(i * (size // LANE) + q, 1), :] for q in range(size // LANE)]
            pick = jnp.concatenate([
                jnp.concatenate([jnp.where(row - first == t_iota, 1.0, 0.0).astype(BF16) for row in tok], axis=1)
                for first in firsts], axis=0)
            at = pl.ds(pl.multiple_of(i * size, size), size)
            value = jnp.dot(pick, rows_u[at, :], preferred_element_type=F32)
            for d in range(2):
                part[d, step] = part[d, step] + value[d * half:(d + 1) * half, :]
            return carry

        lax.fori_loop(0, blocks, body, 0)

    sums = {}
    for step in range(ffn_size):
        combine(step)
        for u in range(subs):
            for d in range(2):
                at = pl.ds(u * sub, sub)
                if step >= 1:
                    sums[d, step - 1, u].wait_recv()
                    value = got[d, step - 1, u] + part[d, step, at, :]
                    if step == last:
                        total[d * half + u * sub:d * half + (u + 1) * sub, :] = value
                    else:
                        got[d, step - 1, u] = value
                if step < last:
                    copy = pltpu.make_async_remote_copy(
                        src_ref=part.at[d, 0, at, :] if step == 0 else got.at[d, step - 1, u], dst_ref=got.at[d, step, u],
                        send_sem=send_a.at[d, step, u], recv_sem=recv_a.at[d, step, u],
                        device_id=peers[d], device_id_type=MESH)
                    copy.start()
                    sums[d, step, u] = copy
    for i in range(own // LANE):
        squares[emb_size - 1, i:i + 1, :] = square_rows(total[i * LANE:(i + 1) * LANE, :])
    shares = share_squares(squares, emb_size, send_b, recv_b)
    for copy in shares:
        copy.wait_recv()
    inv = inverse_rms(squares, emb_size, model_width)
    post = post_ref[...].reshape(1, width).astype(F32)

    def rows(chunk, start, size):
        chunk = lax.rem(chunk + ffn_size * 2, ffn_size)
        return pl.ds(pl.multiple_of(chunk * own + start, size), size)

    for i in range(own // LANE):
        col = jnp.concatenate([column_of(inv[i:i + 1, :])] * (width // LANE), axis=1)
        at = rows(me, i * LANE, LANE)
        out_ref[at, :] = (hid_ref[at, :].astype(F32) + total[i * LANE:(i + 1) * LANE, :] * col * post).astype(BF16)
    spread = []
    for step in range(ffn_size // 2):
        if step >= 1:
            for copy in spread[-2:]:
                copy.wait_recv()
        last = step == (ffn_size - 1) // 2
        for d in range(2):
            chunk = me - step if d == 0 else me + step
            at = rows(chunk, d * own // 2, own // 2) if last else rows(chunk, 0, own)
            spread.append(pltpu.make_async_remote_copy(
                src_ref=out_ref.at[at, :], dst_ref=out_ref.at[at, :],
                send_sem=send_c.at[d, step], recv_sem=recv_c.at[d, step],
                device_id=peers[d], device_id_type=MESH))
            spread[-1].start()
    for copy in spread[-2:]:
        copy.wait_recv()
    for copy in list(sums.values()) + shares + spread:
        copy.wait_send()


def finish(u, tok, hidden, norm_post, ffn_size, emb_size):
    tokens, width = hidden.shape
    rows = tok.size
    own = tokens // ffn_size
    half = own // 2
    subs = 2 if half % 256 == 0 else 1
    vmem = pl.BlockSpec(memory_space=pltpu.VMEM)
    dma = pltpu.SemaphoreType.DMA
    hops = (2, ffn_size - 1, subs)
    return pl.pallas_call(
        functools.partial(finish_kernel, ffn_size, emb_size, width * emb_size),
        out_shape=jax.ShapeDtypeStruct((tokens, width), BF16),
        in_specs=[pl.BlockSpec(memory_space=pl.ANY), vmem, vmem, vmem],
        out_specs=vmem,
        scratch_shapes=[
            pltpu.VMEM((rows, width), BF16),
            pltpu.VMEM((2, ffn_size, half, width), F32),
            pltpu.VMEM(hops + (half // subs, width), F32),
            pltpu.VMEM((own, width), F32),
            pltpu.VMEM((emb_size, own // LANE, LANE), F32),
            dma((rows // 2048,)), dma(hops), dma(hops),
            dma((emb_size - 1,)), dma((emb_size - 1,)),
            dma((2, ffn_size // 2)), dma((2, ffn_size // 2)),
        ],
        compiler_params=pltpu.CompilerParams(collective_id=1, has_side_effects=True, vmem_limit_bytes=VMEM_BYTES),
        cost_estimate=cost(2 * rows * tokens * width, 16e6),
        name='finish',
    )(u, tok, hidden, norm_post)


def down_kernel(seg_ref, gate_ref, g_ref, w_ref, u_ref):
    width = u_ref.shape[1]
    pick = lambda q: lambda: w_ref[q]
    grouped(seg_ref, pl.program_id(0), g_ref, [pick(q) for q in range(w_ref.shape[0])], u_ref)

    @pl.when(pl.program_id(0) == pl.num_programs(0) - 1)
    def scale():
        def body(i, carry):
            for q in range(4):
                hi = i * 4 + q
                col = jnp.concatenate([column_of(gate_ref[pl.ds(hi, 1), :])] * (width // LANE), axis=1)
                at = pl.ds(pl.multiple_of(hi * LANE, LANE), LANE)
                u_ref[at, :] = (u_ref[at, :].astype(F32) * col).astype(BF16)
            return carry

        lax.fori_loop(0, gate_ref.shape[0] // 4, body, 0)


def expert_down(seg, gate, act, w_down):
    rows, ffn = act.shape
    experts, _, width = w_down.shape
    whole = lambda e, seg: (0, 0)
    one = pl.Buffered(1)
    return pl.pallas_call(
        down_kernel,
        out_shape=jax.ShapeDtypeStruct((rows, width), BF16),
        grid_spec=pltpu.PrefetchScalarGridSpec(
            num_scalar_prefetch=1,
            grid=(experts // EXPERT_BATCH,),
            in_specs=[
                pl.BlockSpec(gate.shape, whole, pipeline_mode=one),
                pl.BlockSpec(act.shape, whole, pipeline_mode=one),
                pl.BlockSpec((EXPERT_BATCH, ffn, width), lambda e, seg: (e, 0, 0)),
            ],
            out_specs=pl.BlockSpec((rows, width), whole, pipeline_mode=one),
        ),
        compiler_params=pltpu.CompilerParams(vmem_limit_bytes=VMEM_BYTES),
        cost_estimate=cost(2 * rows * width * ffn, 4 * rows * width),
        name='expert_down',
    )(seg, gate, act, w_down)


def solution(mesh):
    emb_size = mesh.shape['emb']
    ffn_size = mesh.shape['ffn']

    def local_block(hidden, norm_pre, norm_post, w_router, w_gate, w_up, w_down, choice):
        num_tok, local_width = hidden.shape
        experts = w_gate.shape[0]
        top_k = choice.shape[1]
        capacity = 2 * num_tok * top_k // experts
        choice_t = choice.T
        tok, seg, pos, normed, logits = prepare(choice_t, hidden, norm_pre, w_router, capacity, emb_size)
        z = dispatch_up(seg, tok, normed, w_gate, w_up)
        act, gate = exchange(z, logits, choice_t, pos, emb_size)
        u = expert_down(seg, gate, act, w_down)
        return finish(u, tok, hidden, norm_post, ffn_size, emb_size)

    in_specs = (P('dp', 'emb'), P('emb'), P('emb'), P('emb', None), P(None, 'emb', 'ffn'), P(None, 'emb', 'ffn'), P(None, 'ffn', 'emb'), P('dp', None))
    return jax.shard_map(local_block, mesh=mesh, in_specs=in_specs, out_specs=P('dp', 'emb'), check_vma=False)
```
